32 devices in a mesh: leaf: 8 (over z, x), sub: 4 (over y, core).
Axes of the slice: x: 2, y: 2, z: 4, core: 2. Of those that a mesh axis runs over, the one named last changes fastest.
Arguments:
- vectors: bfloat16 [64, 163840], P(None, ('leaf', 'sub')), may hold values from -6 to 6
- row_counts: int32 [32], replicated, may hold values from 3072 to 5120, as said below
- tree_slot: int32 [163840], P(('leaf', 'sub')), may hold values from -1 to 131071, as said below
- leaf_inverse: bfloat16 [512, 256, 256], P(('leaf', 'sub')), may hold values from -0.375 to 0.375
- left_basis: bfloat16 [9, 32, 131072], P(None, None, ('leaf', 'sub')), may hold values from -0.41992188 to 0.41992188
- right_basis: bfloat16 [9, 32, 131072], P(None, None, ('leaf', 'sub')), may hold values from -6 to 6
Outputs:
- applied: bfloat16 [64, 163840], P(None, ('leaf', 'sub'))
The draws below stay inside these ranges and needn't reach their ends.
Inputs may be any that keep to these rules, and one draw needn't show every extreme that they name: The first row_counts[d] of the 5120 slots of owner d are live; the counts sum to 131072. `tree_slot`: live slots hold distinct tree positions covering 0 .. 131071, dead slots hold -1. Tree owner t holds positions t*4096 .. (t+1)*4096 - 1; the live rows of one mesh owner go to one tree owner at most 160 at a time.
All inputs are finite; a program needn't handle non-finite values.
Results may differ from the reference program's by a relative error of at most 0.014.
Values may be sent and summed in bfloat16 or wider, within the bound.
No kernel may reach another device: no remote copies, remote signals or barrier semaphores. Data moves between devices by JAX's collectives and lax.ppermute only.
A program may use at most 64 MiB of HBM per device.

```python
import math
import jax
import jax.numpy as jnp
from jax import lax

VECS = 64
LEAF = 256
RANK = 32
ROWS_DEV = 4096
MESH_CAP = 5120
LEVELS = 9
TOTAL = 131072
N_LEAF = 8
N_SUB = 4
DEVICES = 32


def mesh_plan(key):
    base = jax.random.fold_in(key, 7)
    devices = N_LEAF * N_SUB
    quarter = ROWS_DEV // 4
    k_pair, k_extra, k_owner, k_local = jax.random.split(base, 4)
    pairing = jax.random.permutation(k_pair, devices).astype(jnp.int32)
    half = devices // 2
    extra = jax.random.randint(k_extra, (half,), 0, quarter + 1).astype(jnp.int32)
    extra = extra.at[0].set(quarter)
    delta = jnp.zeros((devices,), jnp.int32).at[pairing[:half]].set(extra).at[pairing[half:]].set(-extra)
    counts = ROWS_DEV + delta
    owner_perm = jax.random.permutation(k_owner, devices).astype(jnp.int32)
    local_perm = jax.vmap(lambda k: jax.random.permutation(k, ROWS_DEV).astype(jnp.int32))(jax.random.split(k_local, devices))
    offsets = jnp.cumsum(counts) - counts
    slot = jnp.arange(devices * MESH_CAP, dtype=jnp.int32)
    owner = slot // MESH_CAP
    within = slot % MESH_CAP
    live = within < counts[owner]
    glob = jnp.where(live, offsets[owner] + within, 0)
    dest = owner_perm[glob % devices]
    place = local_perm[dest, glob // devices]
    tree = jnp.where(live, dest * ROWS_DEV + place, -1).astype(jnp.int32)
    return (counts, tree)


def draw_row_counts(key, part):
    return mesh_plan(key)[0]


def draw_tree_slot(key, part):
    return mesh_plan(key)[1]


def levels(stream_key, extent, cuts, low, largest):
    gain, own = 1.0, jax.random.fold_in(stream_key, 6)
    for axis_at, blocks in cuts:
        steps = jnp.exp(jax.random.uniform(jax.random.fold_in(own, axis_at), (blocks,), jnp.float32, low / len(cuts), largest / len(cuts)))
        gain = gain * jnp.repeat(steps, extent[axis_at] // blocks).reshape([-1 if axis == axis_at else 1 for axis in range(len(extent))])
    return gain


def noise(own_key, dims, spread, reach, cuts=(), held_as=jnp.bfloat16):
    level = levels(own_key, dims, cuts, -0.22, 0.18) if cuts else 1.0
    array = jax.random.normal(own_key, dims, jnp.float32) * spread * level
    return jnp.minimum(jnp.maximum(array, -reach), reach).astype(held_as)


def setup_inputs(seed: int = 0) -> dict:
    streams_of = jax.random.split(jax.random.key(seed), 7)
    return {
        "vectors": noise(streams_of[0], (VECS, DEVICES * MESH_CAP), 1.0, 6.0, ((1, 32),)),
        "row_counts": draw_row_counts(jax.random.fold_in(streams_of[6], 71), 0),
        "tree_slot": draw_tree_slot(jax.random.fold_in(streams_of[6], 71), 0),
        "leaf_inverse": noise(streams_of[3], (TOTAL // LEAF, LEAF, LEAF), LEAF ** -0.5, 0.375, ((0, 32),)),
        "left_basis": noise(streams_of[4], (LEVELS, RANK, TOTAL), 0.07, 0.41992188, ((2, 32),)),
        "right_basis": noise(streams_of[5], (LEVELS, RANK, TOTAL), 1.0, 6.0, ((2, 32),)),
    }


def reference(vectors, row_counts, tree_slot, leaf_inverse, left_basis, right_basis):
    devices = N_LEAF * N_SUB
    total = ROWS_DEV * devices
    slot = jnp.arange(devices * MESH_CAP, dtype=jnp.int32)
    owner = slot // MESH_CAP
    within = slot % MESH_CAP
    live = (within < row_counts[owner]) & (tree_slot >= 0)
    target = jnp.where(live, tree_slot, total).astype(jnp.int32)
    tree = jnp.zeros((VECS, total), jnp.bfloat16).at[:, target].set(vectors, mode='drop')
    blocks = tree.reshape(VECS, total // LEAF, LEAF).astype(jnp.float32)
    field = jnp.einsum('lij,vlj->vli', leaf_inverse.astype(jnp.float32), blocks, precision=lax.Precision.HIGHEST).reshape(VECS, total)
    for level in range(LEVELS):
        size = LEAF * 2 ** level
        nodes = total // size
        rounded = field.astype(jnp.bfloat16).astype(jnp.float32)
        right = right_basis[level].reshape(RANK, nodes, size).astype(jnp.float32)
        coeff = jnp.einsum('rns,vns->nrv', right, rounded.reshape(VECS, nodes, size), precision=lax.Precision.HIGHEST) / math.sqrt(size)
        partner = coeff.reshape(nodes // 2, 2, RANK, VECS)[:, ::-1].reshape(nodes, RANK, VECS)
        partner = partner.astype(jnp.bfloat16).astype(jnp.float32)
        left = left_basis[level].reshape(RANK, nodes, size).astype(jnp.float32)
        field = field - jnp.einsum('rns,nrv->vns', left, partner, precision=lax.Precision.HIGHEST).reshape(VECS, total)
    done = field.astype(jnp.bfloat16)
    picked = done[:, jnp.minimum(target, total - 1)]
    return jnp.where(live[None, :], picked, jnp.zeros_like(picked)).astype(jnp.bfloat16)
```

```python
import functools
import math

import jax
import jax.numpy as jnp
from jax import lax
from jax.experimental import pallas as pl
from jax.experimental.pallas import tpu as pltpu
from jax.sharding import PartitionSpec as P

F32 = jnp.float32
BF16 = jnp.bfloat16
LANES = 128
DIGIT = 64
NT = (((1,), (1,)), ((), ()))
VMEM = pltpu.VMEM
VMEM_LIMIT = 60 * 1024 * 1024


def dot(a, b):
    return jnp.dot(a, b, preferred_element_type=F32)


def dot_nt(a, b):
    return lax.dot_general(a, b, NT, preferred_element_type=F32)


def iota(shape, dim):
    return lax.broadcasted_iota(jnp.int32, shape, dim)


def send_kernel(
    rows, devices, half, count_ref, vec_ref, slot_ref, out_ref, row_ref, part_ref,
    xt, staged, flat, places, posf, sem,
):
    vecs = vec_ref.shape[0]
    blocks = slot_ref.shape[0]
    count = count_ref[0]
    trash = devices * 2 * half
    shift = rows.bit_length() - 1
    owner_id = iota((devices, LANES), 0)
    before = (iota((LANES, LANES), 0) < iota((LANES, LANES), 1)).astype(BF16)
    ones = jnp.ones((LANES, LANES), BF16)
    code_id = iota((2 * LANES, LANES), 0)
    carry = jnp.zeros((devices, LANES), F32)
    pos = jnp.zeros((2 * devices, 2 * LANES), F32)
    for b in range(blocks):
        slot = slot_ref[b : b + 1, :]
        lane = iota((1, LANES), 1) + b * LANES
        live = (lane < count) & (slot >= 0)
        owner = jnp.where(live, slot >> shift, -1)
        local = slot & (rows - 1)
        hot = owner_id == owner
        hot_b = jnp.where(hot, 1.0, 0.0).astype(BF16)
        ranks = dot(hot_b, before) + carry
        carry = carry + dot(hot_b, ones)
        rank = jnp.sum(jnp.where(hot, ranks, 0.0), axis=0, keepdims=True).astype(jnp.int32)
        flat[b : b + 1, :] = jnp.where(live, owner * (2 * half) + rank, trash)
        upper = rank >= half
        row_ref[b : b + 1, :] = jnp.where(live, owner * half + jnp.where(upper, rank - half, rank), 0)
        part_ref[b : b + 1, :] = jnp.where(live, jnp.where(upper, 1, 0), 2)
        code = jnp.where(upper, rank - half + LANES, rank)
        high = ((local >> 6) + 1).astype(F32)
        low = (local & (DIGIT - 1)).astype(F32)
        digits = jnp.concatenate(
            [jnp.where(hot, high, 0.0), jnp.where(hot, low, 0.0)], axis=0
        ).astype(BF16)
        spread = jnp.where(code_id == code, 1.0, 0.0).astype(BF16)
        pos = pos + dot_nt(digits, spread)
    copy = pltpu.make_async_copy(flat, places, sem)
    copy.start()
    for d in range(devices):
        posf[8 * d : 8 * d + 1, :] = pos[d : d + 1, :LANES]
        posf[8 * d + 1 : 8 * d + 2, :] = pos[d : d + 1, LANES:]
        posf[8 * d + 2 : 8 * d + 3, :] = pos[devices + d : devices + d + 1, :LANES]
        posf[8 * d + 3 : 8 * d + 4, :] = pos[devices + d : devices + d + 1, LANES:]

    def turn(b, _):
        x = vec_ref[:, pl.ds(pl.multiple_of(b * LANES, LANES), LANES)].astype(F32)
        xt[pl.ds(pl.multiple_of(b * LANES, LANES), LANES), :] = jnp.concatenate([x, x], axis=0).T
        return 0

    lax.fori_loop(0, blocks, turn, 0, unroll=4)
    copy.wait()

    def move(g, _):
        b = g // (LANES // 32)
        base = (g % (LANES // 32)) * 32
        for u in range(32):
            to = places[b, base + u]
            staged[pl.ds(to, 1), :] = xt[pl.ds(g * 32 + u, 1), :]
        return 0

    lax.fori_loop(0, blocks * (LANES // 32), move, 0)
    lower = iota((half, LANES), 1) < vecs

    def pack(d, _):
        a = staged[pl.ds(pl.multiple_of(d * 2 * half, 8), half), :]
        c = staged[pl.ds(pl.multiple_of(d * 2 * half + half, 8), half), :]
        out_ref[d, pl.ds(0, half), :] = jnp.where(lower, a, c).astype(BF16)
        out_ref[d, pl.ds(half, 8), :] = posf[pl.ds(pl.multiple_of(d * 8, 8), 8), :].astype(BF16)
        return 0

    lax.fori_loop(0, devices, pack, 0)


def tree_kernel(
    local_levels, leaf, rank, arr_ref, inv_hbm, left_hbm, right_hbm, field_ref, b_ref, spot_ref,
    arr, tree, inv, left, right, spots, sems,
):
    devices, chunk, _ = arr_ref.shape
    half = chunk - 8
    rows = field_ref.shape[1]
    vecs = field_ref.shape[0]
    leaves = rows // leaf
    levels = right_hbm.shape[0]
    loads = [
        pltpu.make_async_copy(inv_hbm, inv, sems.at[0]),
        pltpu.make_async_copy(right_hbm, right, sems.at[1]),
        pltpu.make_async_copy(left_hbm.at[pl.ds(0, local_levels)], left, sems.at[2]),
    ]
    for load in loads:
        load.start()

    for d in range(devices):
        pos = arr_ref[d, half:chunk, :].astype(F32)
        high = pos[0:2, :]
        low = pos[2:4, :]
        spot = jnp.where(high > 0.5, (high - 1.0) * DIGIT + low, float(rows)).astype(jnp.int32)
        spot_ref[2 * d : 2 * d + 2, :] = spot
    copy = pltpu.make_async_copy(spot_ref, spots, sems.at[3])
    copy.start()

    def widen(d, _):
        arr[pl.ds(pl.multiple_of(d * half, 8), half), :] = arr_ref[d, pl.ds(0, half), :].astype(F32)
        return 0

    lax.fori_loop(0, devices, widen, 0)

    def clear(i, _):
        tree[pl.ds(pl.multiple_of(i * 64, 64), 64), :] = jnp.zeros((64, LANES), F32)
        return 0

    lax.fori_loop(0, rows // 64, clear, 0)
    copy.wait()
    step = 8

    def place(g, _):
        d = g // (half // step)
        base = (g % (half // step)) * step
        for u in range(step):
            low = spots[2 * d, base + u]
            high = spots[2 * d + 1, base + u]
            row = arr[pl.ds(g * step + u, 1), :]
            tree[pl.ds(low, 1), pl.ds(0, vecs)] = row[:, :vecs]
            tree[pl.ds(high, 1), pl.ds(vecs, vecs)] = row[:, vecs:]
        return 0

    lax.fori_loop(0, devices * (half // step), place, 0)
    loads[0].wait()
    for l in range(leaves):
        block = tree[l * leaf : (l + 1) * leaf, :].astype(BF16)
        turned = dot(inv[l], block).T
        field_ref[:, l * leaf : (l + 1) * leaf] = turned[:vecs] + turned[vecs:]
    loads[1].wait()
    loads[2].wait()
    for k in range(local_levels):
        size = leaf << k
        scale = 1.0 / math.sqrt(size)
        coeff = []
        for n in range(rows // size):
            at = slice(n * size, (n + 1) * size)
            part = dot_nt(field_ref[:, at].astype(BF16), right[k, :, at])
            coeff.append((part * scale).astype(BF16))
        for n in range(rows // size):
            at = slice(n * size, (n + 1) * size)
            field_ref[:, at] = field_ref[:, at] - dot(coeff[n ^ 1], left[k, :, at])
    rounded = field_ref[...].astype(BF16)
    for k in range(local_levels, levels):
        at = slice((k - local_levels) * rank, (k - local_levels + 1) * rank)
        b_ref[:, at] = dot_nt(rounded, right[k])


def gram_kernel(local_levels, rank, left_ref, right_ref, out_ref):
    levels = left_ref.shape[0]
    left = jnp.concatenate([left_ref[k] for k in range(levels)], axis=0)
    right = jnp.concatenate([right_ref[k] for k in range(levels)], axis=0)
    out_ref[...] = dot_nt(left, right)


def back_kernel(
    first, done_levels, rank, field_ref, left_hbm, p_ref, spot_ref, out_ref, done, left, spots, packed, sems
):
    devices, half, _ = out_ref.shape
    vecs, rows = field_ref.shape
    copy = pltpu.make_async_copy(spot_ref, spots, sems.at[0])
    copy.start()
    load = pltpu.make_async_copy(left_hbm.at[pl.ds(first, done_levels)], left, sems.at[1])
    load.start()
    load.wait()
    p = p_ref[...]
    width = 512
    for c in range(rows // width):
        at = slice(c * width, (c + 1) * width)
        basis = jnp.concatenate([left[k, :, at] for k in range(done_levels)], axis=0)
        field = field_ref[:, at] - dot(p, basis)
        for q in range(width // LANES):
            x = field[:, q * LANES : (q + 1) * LANES]
            done[c * width + q * LANES : c * width + (q + 1) * LANES, :] = jnp.concatenate([x, x], axis=0).T
    copy.wait()
    step = 8
    lower = iota((1, LANES), 1) < vecs

    def pick(g, _):
        d = g // (half // step)
        base = (g % (half // step)) * step
        for u in range(step):
            a = done[pl.ds(spots[2 * d, base + u], 1), :]
            c = done[pl.ds(spots[2 * d + 1, base + u], 1), :]
            packed[pl.ds(g * step + u, 1), :] = jnp.where(lower, a, c)
        return 0

    lax.fori_loop(0, devices * (half // step), pick, 0)

    def narrow(d, _):
        out_ref[d, :, :] = packed[pl.ds(pl.multiple_of(d * half, 8), half), :].astype(BF16)
        return 0

    lax.fori_loop(0, devices, narrow, 0)


def final_kernel(ret_ref, row_ref, part_ref, out_ref, ret, picked, places, sem):
    devices, half, _ = ret_ref.shape
    vecs = out_ref.shape[0]
    blocks = row_ref.shape[0]
    copy = pltpu.make_async_copy(row_ref, places, sem)
    copy.start()

    def widen(d, _):
        ret[pl.ds(pl.multiple_of(d * half, 8), half), :] = ret_ref[d, :, :].astype(F32)
        return 0

    lax.fori_loop(0, devices, widen, 0)
    copy.wait()

    def move(g, _):
        b = g // (LANES // 32)
        base = (g % (LANES // 32)) * 32
        for u in range(32):
            picked[pl.ds(g * 32 + u, 1), :] = ret[pl.ds(places[b, base + u], 1), :]
        return 0

    lax.fori_loop(0, blocks * (LANES // 32), move, 0)
    for b in range(blocks):
        x = picked[b * LANES : (b + 1) * LANES, :].T
        part = part_ref[b : b + 1, :]
        value = jnp.where(part == 0, x[:vecs], jnp.where(part == 1, x[vecs:], 0.0))
        out_ref[:, b * LANES : (b + 1) * LANES] = value.astype(BF16)


def merge_kernel(bits, rank, scales, vecs, *refs):
    group = 1 << bits
    ins, (p_ref, out_ref) = refs[:group], refs[group:]
    width = ins[0].shape[1]
    b = [r[:vecs, :].astype(F32) for r in ins]
    gram = [r[vecs:, :].astype(F32) for r in ins]
    for step in range(bits):
        at = slice(step * rank, (step + 1) * rank)
        p = [(b[x ^ 1][:, at] * scales[step]).astype(BF16) for x in range(len(b))]
        p_ref[:, at] = p[0]
        b = [b[x] - dot(p[x], gram[x][at, :].astype(BF16)) for x in range(len(b))]
        b = [b[x] + b[x + 1] for x in range(0, len(b), 2)]
        gram = [gram[x] + gram[x + 1] for x in range(0, len(gram), 2)]
    if width > bits * rank:
        out_ref[:vecs, :] = b[0][:, bits * rank :].astype(BF16)
        out_ref[vecs:, :] = gram[0][bits * rank :, bits * rank :].astype(BF16)
    else:
        out_ref[...] = jnp.zeros(out_ref.shape, BF16)


def full(shape, dtype):
    return jax.ShapeDtypeStruct(shape, dtype)


def vmem():
    return pl.BlockSpec(memory_space=VMEM)


def anywhere():
    return pl.BlockSpec(memory_space=pl.ANY)


def params():
    return pltpu.CompilerParams(vmem_limit_bytes=VMEM_LIMIT)


def flipped(block, axis, mask):
    count = lax.axis_size(axis)
    return lax.ppermute(block, axis, [(i, i ^ mask) for i in range(count)])


def body(vectors, row_counts, tree_slot, leaf_inverse, left_basis, right_basis):
    vecs, slots = vectors.shape
    leaves, leaf = leaf_inverse.shape[0], leaf_inverse.shape[1]
    rows = leaves * leaf
    levels, rank = left_basis.shape[0], left_basis.shape[1]
    n_leaf = lax.axis_size("leaf")
    n_sub = lax.axis_size("sub")
    devices = n_leaf * n_sub
    sub_bits = n_sub.bit_length() - 1
    leaf_bits = n_leaf.bit_length() - 1
    cross = sub_bits + leaf_bits
    local_levels = levels - cross
    cap = (slots + devices - 1) // devices
    half = ((cap + 1) // 2 + 7) // 8 * 8
    blocks = slots // LANES
    axes = ("leaf", "sub")
    if vecs * 2 != LANES or half > LANES or slots % LANES or rows != 1 << (rows.bit_length() - 1):
        raise ValueError("unsupported sizes")
    me = lax.axis_index("leaf") * n_sub + lax.axis_index("sub")
    count = lax.dynamic_slice(row_counts, (me,), (1,))

    outgoing, row_of, part_of = pl.pallas_call(
        functools.partial(send_kernel, rows, devices, half),
        out_shape=(
            full((devices, half + 8, LANES), BF16),
            full((blocks, LANES), jnp.int32),
            full((blocks, LANES), jnp.int32),
        ),
        in_specs=[pl.BlockSpec(memory_space=pltpu.SMEM), vmem(), vmem()],
        out_specs=(vmem(), vmem(), vmem()),
        scratch_shapes=[
            VMEM((slots, LANES), F32),
            VMEM((devices * 2 * half + 8, LANES), F32),
            VMEM((blocks, LANES), jnp.int32),
            pltpu.SMEM((blocks, LANES), jnp.int32),
            VMEM((8 * devices, LANES), F32),
            pltpu.SemaphoreType.DMA,
        ],
        compiler_params=params(),
        name="send",
    )(count, vectors, tree_slot.reshape(blocks, LANES))

    arrived = lax.all_to_all(outgoing, axes, split_axis=0, concat_axis=0, tiled=True)

    gram = pl.pallas_call(
        functools.partial(gram_kernel, local_levels, rank),
        out_shape=full((cross * rank, cross * rank), F32),
        in_specs=[vmem(), vmem()],
        out_specs=vmem(),
        compiler_params=params(),
        name="gram",
    )(left_basis[local_levels:], right_basis[local_levels:])

    field, partial_b, spots = pl.pallas_call(
        functools.partial(tree_kernel, local_levels, leaf, rank),
        out_shape=(
            full((vecs, rows), F32),
            full((vecs, cross * rank), F32),
            full((2 * devices, LANES), jnp.int32),
        ),
        in_specs=[vmem(), anywhere(), anywhere(), anywhere()],
        out_specs=(vmem(), vmem(), vmem()),
        scratch_shapes=[
            VMEM((devices * half, LANES), F32),
            VMEM((rows + 8, LANES), F32),
            VMEM((leaves, leaf, leaf), BF16),
            VMEM((local_levels, rank, rows), BF16),
            VMEM((levels, rank, rows), BF16),
            pltpu.SMEM((2 * devices, LANES), jnp.int32),
            pltpu.SemaphoreType.DMA((4,)),
        ],
        compiler_params=params(),
        name="tree",
    )(arrived, leaf_inverse, left_basis, right_basis)

    stages = []
    for axis, n_bits in (("sub", sub_bits), ("leaf", leaf_bits)):
        bit = 0
        while bit < n_bits:
            take = min(2, n_bits - bit)
            stages.append((axis, bit, take))
            bit += take
    message = jnp.concatenate([partial_b, gram], axis=0).astype(BF16)
    level = local_levels
    solved = []
    for axis, bit, take in stages:
        group = [message]
        for mask in range(1, 1 << take):
            group.append(flipped(message, axis, mask << bit))
        scales = [1.0 / math.sqrt(leaf << (level + s)) for s in range(take)]
        left_over = message.shape[1] - take * rank
        shape = (vecs + left_over, left_over) if left_over else (16, LANES)
        p, message = pl.pallas_call(
            functools.partial(merge_kernel, take, rank, scales, vecs),
            out_shape=(full((vecs, take * rank), BF16), full(shape, BF16)),
            in_specs=[vmem()] * len(group),
            out_specs=(vmem(), vmem()),
            compiler_params=params(),
            name="merge",
        )(*group)
        solved.append(p)
        level += take
    partner = jnp.concatenate(solved, axis=1)

    back = pl.pallas_call(
        functools.partial(back_kernel, local_levels, cross, rank),
        out_shape=full((devices, half, LANES), BF16),
        in_specs=[vmem(), anywhere(), vmem(), vmem()],
        out_specs=vmem(),
        scratch_shapes=[
            VMEM((rows + 8, LANES), F32),
            VMEM((cross, rank, rows), BF16),
            pltpu.SMEM((2 * devices, LANES), jnp.int32),
            VMEM((devices * half, LANES), F32),
            pltpu.SemaphoreType.DMA((2,)),
        ],
        compiler_params=params(),
        name="back",
    )(field, left_basis, partner, spots)

    returned = lax.all_to_all(back, axes, split_axis=0, concat_axis=0, tiled=True)

    return pl.pallas_call(
        final_kernel,
        out_shape=full((vecs, slots), BF16),
        in_specs=[vmem(), vmem(), vmem()],
        out_specs=vmem(),
        scratch_shapes=[
            VMEM((devices * half, LANES), F32),
            VMEM((slots, LANES), F32),
            pltpu.SMEM((blocks, LANES), jnp.int32),
            pltpu.SemaphoreType.DMA,
        ],
        compiler_params=params(),
        name="final",
    )(returned, row_of, part_of)


def solution(mesh):
    in_specs = (
        P(None, ("leaf", "sub")),
        P(),
        P(("leaf", "sub")),
        P(("leaf", "sub"), None, None),
        P(None, None, ("leaf", "sub")),
        P(None, None, ("leaf", "sub")),
    )
    out_specs = P(None, ("leaf", "sub"))
    return jax.shard_map(body, mesh=mesh, in_specs=in_specs, out_specs=out_specs, check_vma=False)
```

```python
import functools
import math

import jax
import jax.numpy as jnp
from jax import lax
from jax.experimental import pallas as pl
from jax.experimental.pallas import tpu as pltpu
from jax.sharding import PartitionSpec as P

F32 = jnp.float32
BF16 = jnp.bfloat16
I32 = jnp.int32
LANES = 128
DIGIT = 64
NT = (((1,), (1,)), ((), ()))
VMEM = pltpu.VMEM
SMEM = pltpu.SMEM
CHUNKS = 1


def dot(a, b):
    return jnp.dot(a, b, preferred_element_type=F32)


def dot_nt(a, b):
    return lax.dot_general(a, b, NT, preferred_element_type=F32)


def iota(shape, dim):
    return lax.broadcasted_iota(I32, shape, dim)


def rows_at(start, size):
    return pl.ds(pl.multiple_of(start, 8), size)


def send_kernel(rows, vecs, chunks, half, n_sub, counts_ref, vec_ref, slot_ref, *refs):
    outs = refs[:chunks]
    row_ref, part_ref, xt, staged, flat, places, posf, sem = refs[chunks:]
    devices = outs[0].shape[0]
    width = vecs // chunks
    parts = LANES // width
    blocks = slot_ref.shape[0]
    count = counts_ref[lax.axis_index("leaf") * n_sub + lax.axis_index("sub")]
    trash = devices * parts * half
    shift = rows.bit_length() - 1
    owner_id = iota((devices, LANES), 0)
    before = (iota((LANES, LANES), 0) < iota((LANES, LANES), 1)).astype(BF16)
    ones = jnp.ones((LANES, LANES), BF16)
    code_id = iota((parts * LANES, LANES), 0)
    carry = jnp.zeros((devices, LANES), F32)
    pos = jnp.zeros((2 * devices, parts * LANES), F32)
    for b in range(blocks):
        slot = slot_ref[b : b + 1, :]
        lane = iota((1, LANES), 1) + b * LANES
        live = (lane < count) & (slot >= 0)
        owner = jnp.where(live, slot >> shift, -1)
        local = slot & (rows - 1)
        hot = owner_id == owner
        hot_b = jnp.where(hot, 1.0, 0.0).astype(BF16)
        ranks = dot(hot_b, before) + carry
        carry = carry + dot(hot_b, ones)
        rank = jnp.sum(jnp.where(hot, ranks, 0.0), axis=0, keepdims=True).astype(I32)
        flat[b : b + 1, :] = jnp.where(live, owner * (parts * half) + rank, trash)
        part = jnp.zeros((1, LANES), I32)
        for q in range(1, parts):
            part = part + jnp.where(rank >= q * half, 1, 0)
        inner = rank - part * half
        row_ref[b : b + 1, :] = jnp.where(live, owner * half + inner, 0)
        part_ref[b : b + 1, :] = jnp.where(live, part, parts)
        high = ((local >> 6) + 1).astype(F32)
        low = (local & (DIGIT - 1)).astype(F32)
        digits = jnp.concatenate(
            [jnp.where(hot, high, 0.0), jnp.where(hot, low, 0.0)], axis=0
        ).astype(BF16)
        spread = jnp.where(code_id == part * LANES + inner, 1.0, 0.0).astype(BF16)
        pos = pos + dot_nt(digits, spread)
    copy = pltpu.make_async_copy(flat, places, sem)
    copy.start()
    for d in range(devices):
        for q in range(parts):
            at = slice(q * LANES, (q + 1) * LANES)
            posf[8 * d + q : 8 * d + q + 1, :] = pos[d : d + 1, at]
            posf[8 * d + parts + q : 8 * d + parts + q + 1, :] = pos[devices + d : devices + d + 1, at]

    def turn(b, _):
        x = vec_ref[:, pl.ds(pl.multiple_of(b * LANES, LANES), LANES)].astype(F32)
        xt[rows_at(b * LANES, LANES), :] = jnp.concatenate([x, x], axis=0).T
        return 0

    lax.fori_loop(0, blocks, turn, 0, unroll=8)
    copy.wait()

    def move(b, _):
        for u in range(LANES):
            staged[pl.ds(places[b, u], 1), :] = xt[pl.ds(b * LANES + u, 1), :]
        return 0

    lax.fori_loop(0, blocks, move, 0)
    group = iota((half, LANES), 1) // width

    def pack(d, _):
        direct = [staged[rows_at((d * parts + q) * half, half), :] for q in range(parts)]
        moved = [pltpu.roll(x, width, 1) for x in direct] if chunks == 2 else direct
        for c in range(chunks):
            packed = None
            for q in range(parts):
                x = direct[q] if q % chunks == c else moved[q]
                packed = x if packed is None else jnp.where(group == q, x, packed)
            outs[c][d, pl.ds(0, half), :] = packed.astype(BF16)
        outs[0][d, pl.ds(half, 8), :] = posf[rows_at(d * 8, 8), :].astype(BF16)
        return 0

    lax.fori_loop(0, devices, pack, 0)


def band_tiles(halves, levels):
    tiles = [("b", h, k) for k in range(levels) for h in range(halves)]
    return tiles + [("g", j, k) for j in range(levels) for k in range(j + 1, levels)]


def band_rows(halves, levels, rank):
    return (len(band_tiles(halves, levels)) + 3) // 4 * rank


def pack_bands(ref, b, gram, rank, halves, levels):
    tiles = band_tiles(halves, levels)
    blank = jnp.zeros((rank, rank), F32)
    for r in range(0, len(tiles), 4):
        band = []
        for kind, x, k in tiles[r : r + 4]:
            at = slice(k * rank, (k + 1) * rank)
            band.append(b[x * rank : (x + 1) * rank, at] if kind == "b" else gram[x][:, at])
        band += [blank] * (4 - len(band))
        ref[r // 4 * rank : (r // 4 + 1) * rank, :] = jnp.concatenate(band, axis=1).astype(BF16)


def unpack_bands(value, rank, halves, levels):
    tiles = band_tiles(halves, levels)
    found = {}
    for t, key in enumerate(tiles):
        found[key] = value[t // 4 * rank : (t // 4 + 1) * rank, t % 4 * rank : (t % 4 + 1) * rank]
    b = jnp.concatenate(
        [
            jnp.concatenate([found["b", h, k] for k in range(levels)], axis=1)
            for h in range(halves)
        ],
        axis=0,
    )
    blank = jnp.zeros((rank, rank), F32)
    gram = [
        jnp.concatenate([found["g", j, k] if k > j else blank for k in range(levels)], axis=1)
        for j in range(levels)
    ]
    return b, gram


def tree_kernel(
    local_levels, leaf, rank, arr_ref, pos_ref, inv, left, right, gram_ref,
    field_ref, message_ref, spot_ref, arr, tree, spots, sem,
):
    devices = arr_ref.shape[0]
    vecs, rows = field_ref.shape
    parts = LANES // vecs
    half = arr.shape[0] // devices
    leaves = rows // leaf
    levels = right.shape[0]
    for d in range(devices):
        pos = pos_ref[d, half : half + 8, :].astype(F32)
        high = pos[0:parts, :]
        low = pos[parts : 2 * parts, :]
        spot = jnp.where(high > 0.5, (high - 1.0) * DIGIT + low, float(rows)).astype(I32)
        spot_ref[parts * d : parts * (d + 1), :] = spot
    copy = pltpu.make_async_copy(spot_ref, spots, sem)
    copy.start()

    def widen(d, _):
        arr[rows_at(d * half, half), :] = arr_ref[d, pl.ds(0, half), :].astype(F32)
        return 0

    lax.fori_loop(0, devices, widen, 0)

    def clear(i, _):
        tree[rows_at(i * 128, 128), :] = jnp.zeros((128, LANES), F32)
        return 0

    lax.fori_loop(0, rows // 128, clear, 0)
    copy.wait()

    def place(d, _):
        for u in range(half):
            row = arr[pl.ds(d * half + u, 1), :]
            for q in range(parts):
                at = pl.ds(spots[parts * d + q, u], 1)
                tree[at, pl.ds(q * vecs, vecs)] = row[:, q * vecs : (q + 1) * vecs]
        return 0

    lax.fori_loop(0, devices, place, 0)
    for l in range(leaves):
        block = tree[l * leaf : (l + 1) * leaf, :].astype(BF16)
        turned = dot(inv[l], block).T
        total = turned[:vecs]
        for q in range(1, parts):
            total = total + turned[q * vecs : (q + 1) * vecs]
        field_ref[:, l * leaf : (l + 1) * leaf] = total
    for k in range(local_levels):
        size = leaf << k
        scale = 1.0 / math.sqrt(size)
        coeff = []
        for n in range(rows // size):
            at = slice(n * size, (n + 1) * size)
            part = dot_nt(field_ref[:, at].astype(BF16), right[k, :, at])
            coeff.append((part * scale).astype(BF16))
        for n in range(rows // size):
            at = slice(n * size, (n + 1) * size)
            field_ref[:, at] = field_ref[:, at] - dot(coeff[n ^ 1], left[k, :, at])
    rounded = field_ref[...].astype(BF16)
    cross = levels - local_levels
    b = jnp.concatenate([dot_nt(rounded, right[k]) for k in range(local_levels, levels)], axis=1)
    gram = [gram_ref[j * rank : (j + 1) * rank, :] for j in range(cross)]
    pack_bands(message_ref, b, gram, rank, vecs // rank, cross)


def gram_kernel(first, left, right, out_ref):
    levels = left.shape[0]
    lhs = jnp.concatenate([left[k] for k in range(first, levels)], axis=0)
    rhs = jnp.concatenate([right[k] for k in range(first, levels)], axis=0)
    out_ref[...] = dot_nt(lhs, rhs)


def merge_kernel(bits, rank, scales, vecs, levels, *refs):
    group = 1 << bits
    p_ref = refs[group]
    halves = vecs // rank
    found = [unpack_bands(r[...].astype(F32), rank, halves, levels) for r in refs[:group]]
    b = [f[0] for f in found]
    gram = [f[1] for f in found]
    for step in range(bits):
        at = slice(step * rank, (step + 1) * rank)
        p = [(b[x ^ 1][:, at] * scales[step]).astype(BF16) for x in range(len(b))]
        p_ref[:, at] = p[0]
        if step + 1 < levels:
            b = [b[x] - dot(p[x], gram[x][step].astype(BF16)) for x in range(len(b))]
            b = [b[x] + b[x + 1] for x in range(0, len(b), 2)]
            gram = [
                [u + v for u, v in zip(gram[x], gram[x + 1])] for x in range(0, len(gram), 2)
            ]
    if levels > bits:
        keep = slice(bits * rank, levels * rank)
        rest = [g[:, keep] for g in gram[0][bits:]]
        pack_bands(refs[group + 1], b[0][:, keep], rest, rank, halves, levels - bits)


def back_kernel(first, rank, n_solved, field_ref, left, spot_ref, *refs):
    solved = refs[:n_solved]
    out_ref, done, spots, packed, sem = refs[n_solved:]
    devices, half, _ = out_ref.shape
    vecs, rows = field_ref.shape
    parts = LANES // vecs
    levels = left.shape[0]
    copy = pltpu.make_async_copy(spot_ref, spots, sem)
    copy.start()
    p = jnp.concatenate([r[...] for r in solved], axis=1)
    wide = 512
    for c in range(rows // wide):
        at = slice(c * wide, (c + 1) * wide)
        basis = jnp.concatenate([left[k, :, at] for k in range(first, levels)], axis=0)
        field = field_ref[:, at] - dot(p, basis)
        for q in range(wide // LANES):
            x = field[:, q * LANES : (q + 1) * LANES]
            low = c * wide + q * LANES
            done[low : low + LANES, :] = jnp.concatenate([x] * parts, axis=0).T
    copy.wait()
    group = iota((1, LANES), 1) // vecs

    def pick(d, _):
        for u in range(half):
            row = done[pl.ds(spots[parts * d, u], 1), :]
            for q in range(1, parts):
                row = jnp.where(group == q, done[pl.ds(spots[parts * d + q, u], 1), :], row)
            packed[pl.ds(d * half + u, 1), :] = row
        return 0

    lax.fori_loop(0, devices, pick, 0)

    def narrow(d, _):
        out_ref[d, :, :] = packed[rows_at(d * half, half), :].astype(BF16)
        return 0

    lax.fori_loop(0, devices, narrow, 0)


def final_kernel(ret_ref, row_ref, part_ref, out_ref, ret, picked, places, sem):
    devices, half, _ = ret_ref.shape
    vecs = out_ref.shape[0]
    parts = LANES // vecs
    blocks = row_ref.shape[0]
    copy = pltpu.make_async_copy(row_ref, places, sem)
    copy.start()

    def widen(d, _):
        ret[rows_at(d * half, half), :] = ret_ref[d, :, :].astype(F32)
        return 0

    lax.fori_loop(0, devices, widen, 0)
    copy.wait()

    def move(b, _):
        for u in range(LANES):
            picked[pl.ds(b * LANES + u, 1), :] = ret[pl.ds(places[b, u], 1), :]
        return 0

    lax.fori_loop(0, blocks, move, 0)
    for b in range(blocks):
        x = picked[b * LANES : (b + 1) * LANES, :].T
        part = part_ref[b : b + 1, :]
        value = jnp.zeros((vecs, LANES), F32)
        for q in range(parts):
            value = jnp.where(part == q, x[q * vecs : (q + 1) * vecs], value)
        out_ref[:, b * LANES : (b + 1) * LANES] = value.astype(BF16)


def full(shape, dtype):
    return jax.ShapeDtypeStruct(shape, dtype)


def vmem():
    return pl.BlockSpec(memory_space=VMEM)


def call(kernel, name, mib, flops, out_shape, in_specs, out_specs, scratch_shapes=()):
    return pl.pallas_call(
        kernel,
        out_shape=out_shape,
        in_specs=in_specs,
        out_specs=out_specs,
        scratch_shapes=scratch_shapes,
        compiler_params=pltpu.CompilerParams(vmem_limit_bytes=mib << 20),
        cost_estimate=pl.CostEstimate(flops=flops, bytes_accessed=1 << 20, transcendentals=0),
        name=name,
    )


def flipped(block, axis, mask):
    count = lax.axis_size(axis)
    return lax.ppermute(block, axis, [(i, i ^ mask) for i in range(count)])


def body(vectors, row_counts, tree_slot, leaf_inverse, left_basis, right_basis):
    vecs, slots = vectors.shape
    leaves, leaf = leaf_inverse.shape[0], leaf_inverse.shape[1]
    rows = leaves * leaf
    levels, rank = left_basis.shape[0], left_basis.shape[1]
    n_leaf = lax.axis_size("leaf")
    n_sub = lax.axis_size("sub")
    devices = n_leaf * n_sub
    sub_bits = n_sub.bit_length() - 1
    leaf_bits = n_leaf.bit_length() - 1
    cross = sub_bits + leaf_bits
    local_levels = levels - cross
    cap = (slots + devices - 1) // devices
    blocks = slots // LANES
    axes = ("leaf", "sub")
    chunks = CHUNKS
    width = vecs // chunks
    parts = LANES // width
    half = ((cap + parts - 1) // parts + 7) // 8 * 8
    if vecs * 2 != LANES or half > LANES or slots % LANES or rows & (rows - 1):
        raise ValueError("unsupported sizes")

    smem = pl.BlockSpec(memory_space=SMEM)
    outgoing = call(
        functools.partial(send_kernel, rows, vecs, chunks, half, n_sub),
        "send",
        20,
        1 << 30,
        tuple(
            full((devices, half + 8 if c == 0 else half, LANES), BF16) for c in range(chunks)
        )
        + (full((blocks, LANES), I32), full((blocks, LANES), I32)),
        [smem, vmem(), vmem()],
        (vmem(),) * (chunks + 2),
        [
            VMEM((slots, LANES), F32),
            VMEM((devices * parts * half + 8, LANES), F32),
            VMEM((blocks, LANES), I32),
            SMEM((blocks, LANES), I32),
            VMEM((8 * devices, LANES), F32),
            pltpu.SemaphoreType.DMA,
        ],
    )(row_counts, vectors, tree_slot.reshape(blocks, LANES))
    row_of, part_of = outgoing[chunks:]

    def exchange(x):
        return lax.all_to_all(x, axes, split_axis=0, concat_axis=0, tiled=True)

    arrived = [exchange(x) for x in outgoing[:chunks]]

    gram = call(
        functools.partial(gram_kernel, local_levels),
        "gram",
        8,
        1 << 30,
        full((cross * rank, cross * rank), F32),
        [vmem(), vmem()],
        vmem(),
    )(left_basis, right_basis)

    stages = []
    for axis, n_bits in (("sub", sub_bits), ("leaf", leaf_bits)):
        bit = 0
        while bit < n_bits:
            take = min(2, n_bits - bit)
            stages.append((axis, bit, take))
            bit += take
    halves = width // rank
    results = []
    for c in range(chunks):
        field, message, spots = call(
            functools.partial(tree_kernel, local_levels, leaf, rank),
            "tree",
            20,
            1 << 30,
            (
                full((width, rows), F32),
                full((band_rows(halves, cross, rank), LANES), BF16),
                full((parts * devices, LANES), I32),
            ),
            [vmem()] * 6,
            (vmem(), vmem(), vmem()),
            [
                VMEM((devices * half, LANES), F32),
                VMEM((rows + 8, LANES), F32),
                SMEM((parts * devices, LANES), I32),
                pltpu.SemaphoreType.DMA,
            ],
        )(arrived[c], arrived[0], leaf_inverse, left_basis, right_basis, gram)

        level = local_levels
        solved = []
        for axis, bit, take in stages:
            group = [message]
            for mask in range(1, 1 << take):
                group.append(flipped(message, axis, mask << bit))
            scales = [1.0 / math.sqrt(leaf << (level + s)) for s in range(take)]
            left_over = levels - level - take
            shapes = [full((width, take * rank), BF16)]
            if left_over:
                shapes.append(full((band_rows(halves, left_over, rank), LANES), BF16))
            out = call(
                functools.partial(merge_kernel, take, rank, scales, width, levels - level),
                "merge",
                4,
                1 << 24,
                tuple(shapes),
                [vmem()] * len(group),
                (vmem(),) * len(shapes),
            )(*group)
            solved.append(out[0])
            message = out[-1]
            level += take

        back = call(
            functools.partial(back_kernel, local_levels, rank, len(solved)),
            "back",
            14,
            1 << 30,
            full((devices, half, LANES), BF16),
            [vmem()] * (3 + len(solved)),
            vmem(),
            [
                VMEM((rows + 8, LANES), F32),
                SMEM((parts * devices, LANES), I32),
                VMEM((devices * half, LANES), F32),
                pltpu.SemaphoreType.DMA,
            ],
        )(field, left_basis, spots, *solved)
        returned = exchange(back)
        results.append(
            call(
                final_kernel,
                "final",
                14,
                1 << 30,
                full((width, slots), BF16),
                [vmem(), vmem(), vmem()],
                vmem(),
                [
                    VMEM((devices * half, LANES), F32),
                    VMEM((slots, LANES), F32),
                    SMEM((blocks, LANES), I32),
                    pltpu.SemaphoreType.DMA,
                ],
            )(returned, row_of, part_of)
        )
    return results[0] if chunks == 1 else jnp.concatenate(results, axis=0)


def solution(mesh):
    in_specs = (
        P(None, ("leaf", "sub")),
        P(),
        P(("leaf", "sub")),
        P(("leaf", "sub"), None, None),
        P(None, None, ("leaf", "sub")),
        P(None, None, ("leaf", "sub")),
    )
    out_specs = P(None, ("leaf", "sub"))
    return jax.shard_map(body, mesh=mesh, in_specs=in_specs, out_specs=out_specs, check_vma=False)
```

```python
import functools
import math

import jax
import jax.numpy as jnp
from jax import lax
from jax.experimental import pallas as pl
from jax.experimental.pallas import tpu as pltpu
from jax.sharding import PartitionSpec as P

F32 = jnp.float32
BF16 = jnp.bfloat16
I32 = jnp.int32
LANES = 128
DIGIT = 64
NT = (((1,), (1,)), ((), ()))
VMEM = pltpu.VMEM
SMEM = pltpu.SMEM
FINAL_UNROLL = 40
PLACE_UNROLL = 32
PICK_UNROLL = 32
SEND_UNROLL = 1


def dot(a, b):
    return jnp.dot(a, b, preferred_element_type=F32)


def dot_nt(a, b):
    return lax.dot_general(a, b, NT, preferred_element_type=F32)


def iota(shape, dim):
    return lax.broadcasted_iota(I32, shape, dim)


def rows_at(start, size):
    return pl.ds(pl.multiple_of(start, 8), size)


def send_kernel(
    rows, vecs, half, n_sub, first, counts_hbm, vec_hbm, slot_hbm, left_hbm, right_hbm,
    out_ref, row_ref, part_ref, gram_ref,
    counts, vec, slots, left, right, xt, staged, flat, places, owners, codes, pos, posf, sems,
):
    devices = out_ref.shape[0]
    parts = LANES // vecs
    blocks = slots.shape[0]
    levels = left_hbm.shape[0]
    cross = levels - first
    loads = [
        pltpu.make_async_copy(counts_hbm, counts, sems.at[0]),
        pltpu.make_async_copy(slot_hbm, slots, sems.at[1]),
        pltpu.make_async_copy(vec_hbm, vec, sems.at[2]),
        pltpu.make_async_copy(left_hbm.at[pl.ds(first, cross)], left, sems.at[3]),
        pltpu.make_async_copy(right_hbm.at[pl.ds(first, cross)], right, sems.at[4]),
    ]
    for load in loads:
        load.start()
    trash = devices * parts * half
    shift = rows.bit_length() - 1
    owner_id = iota((devices, LANES), 0)
    before = (iota((LANES, LANES), 0) < iota((LANES, LANES), 1)).astype(BF16)
    ones = jnp.ones((LANES, LANES), BF16)
    carry = jnp.zeros((devices, LANES), F32)
    loads[0].wait()
    loads[1].wait()
    count = counts[lax.axis_index("leaf") * n_sub + lax.axis_index("sub")]
    for b in range(blocks):
        slot = slots[b : b + 1, :]
        lane = iota((1, LANES), 1) + b * LANES
        live = (lane < count) & (slot >= 0)
        owner = jnp.where(live, slot >> shift, -1)
        hot = owner_id == owner
        hot_b = jnp.where(hot, 1.0, 0.0).astype(BF16)
        ranks = dot(hot_b, before) + carry
        carry = carry + dot(hot_b, ones)
        rank = jnp.sum(jnp.where(hot, ranks, 0.0), axis=0, keepdims=True).astype(I32)
        flat[b : b + 1, :] = jnp.where(live, owner * (parts * half) + rank, trash)
        part = jnp.zeros((1, LANES), I32)
        for q in range(1, parts):
            part = part + jnp.where(rank >= q * half, 1, 0)
        inner = rank - part * half
        row_ref[b : b + 1, :] = jnp.where(live, owner * half + inner, 0)
        part_ref[b : b + 1, :] = jnp.where(live, part, parts)
        owners[b : b + 1, :] = owner
        codes[b : b + 1, :] = part * LANES + inner
    copy = pltpu.make_async_copy(flat, places, sems.at[5])
    copy.start()
    for load in loads[2:]:
        load.wait()
    pos[...] = jnp.zeros(pos.shape, F32)
    gram_ref[...] = jnp.zeros(gram_ref.shape, F32)
    code_id = iota((parts * LANES, LANES), 0)
    tile = 256
    tiles = rows // tile

    def turn(b, _):
        at = pl.multiple_of(b * LANES, LANES)
        x = vec[:, pl.ds(at, LANES)].astype(F32)
        xt[pl.ds(at, LANES), :] = jnp.concatenate([x] * parts, axis=0).T
        return 0

    lax.fori_loop(0, blocks, turn, 0, unroll=8)
    copy.wait()

    def move(i, _):
        digits, spread = [], []
        for s in range(2):
            b = 2 * i + s
            hot = owner_id == owners[pl.ds(b, 1), :]
            local = slots[pl.ds(b, 1), :] & (rows - 1)
            high = ((local >> 6) + 1).astype(F32)
            low = (local & (DIGIT - 1)).astype(F32)
            digits.append(
                jnp.concatenate([jnp.where(hot, high, 0.0), jnp.where(hot, low, 0.0)], axis=0)
            )
            spread.append(jnp.where(code_id == codes[pl.ds(b, 1), :], 1.0, 0.0))
            for u in range(LANES):
                staged[pl.ds(places[b, u], 1), :] = xt[pl.ds(b * LANES + u, 1), :]
        pos[...] = pos[...] + dot_nt(
            jnp.concatenate(digits, axis=1).astype(BF16),
            jnp.concatenate(spread, axis=1).astype(BF16),
        )
        at = pl.ds(pl.multiple_of(jnp.minimum(i, tiles - 1) * tile, tile), tile)
        keep = jnp.where(i < tiles, 1.0, 0.0)
        lhs = jnp.concatenate([left[k, :, at] for k in range(cross)], axis=0)
        rhs = jnp.concatenate([right[k, :, at] for k in range(cross)], axis=0)
        gram_ref[...] = gram_ref[...] + dot_nt(lhs, rhs) * keep
        return 0

    lax.fori_loop(0, blocks // 2, move, 0, unroll=SEND_UNROLL)
    for d in range(devices):
        for q in range(parts):
            at = slice(q * LANES, (q + 1) * LANES)
            posf[8 * d + q : 8 * d + q + 1, :] = pos[d : d + 1, at]
            posf[8 * d + parts + q : 8 * d + parts + q + 1, :] = pos[devices + d : devices + d + 1, at]
    group = iota((half, LANES), 1) // vecs

    def pack(d, _):
        packed = staged[rows_at(d * parts * half, half), :]
        for q in range(1, parts):
            packed = jnp.where(group == q, staged[rows_at((d * parts + q) * half, half), :], packed)
        out_ref[d, pl.ds(0, half), :] = packed.astype(BF16)
        out_ref[d, pl.ds(half, 8), :] = posf[rows_at(d * 8, 8), :].astype(BF16)
        return 0

    lax.fori_loop(0, devices, pack, 0)


def band_tiles(halves, levels):
    tiles = [("b", h, k) for k in range(levels) for h in range(halves)]
    return tiles + [("g", j, k) for j in range(levels) for k in range(j + 1, levels)]


def band_rows(halves, levels, rank):
    return (len(band_tiles(halves, levels)) + 3) // 4 * rank


def pack_bands(ref, b, gram, rank, halves, levels):
    tiles = band_tiles(halves, levels)
    blank = jnp.zeros((rank, rank), F32)
    for r in range(0, len(tiles), 4):
        band = []
        for kind, x, k in tiles[r : r + 4]:
            at = slice(k * rank, (k + 1) * rank)
            band.append(b[x * rank : (x + 1) * rank, at] if kind == "b" else gram[x][:, at])
        band += [blank] * (4 - len(band))
        ref[r // 4 * rank : (r // 4 + 1) * rank, :] = jnp.concatenate(band, axis=1).astype(BF16)


def unpack_bands(value, rank, halves, levels):
    tiles = band_tiles(halves, levels)
    found = {}
    for t, key in enumerate(tiles):
        found[key] = value[t // 4 * rank : (t // 4 + 1) * rank, t % 4 * rank : (t % 4 + 1) * rank]
    b = jnp.concatenate(
        [
            jnp.concatenate([found["b", h, k] for k in range(levels)], axis=1)
            for h in range(halves)
        ],
        axis=0,
    )
    blank = jnp.zeros((rank, rank), F32)
    gram = [
        jnp.concatenate([found["g", j, k] if k > j else blank for k in range(levels)], axis=1)
        for j in range(levels)
    ]
    return b, gram


def tree_kernel(
    local_levels, leaf, rank, arr_ref, inv_hbm, left_hbm, right_hbm, gram_ref,
    field_ref, message_ref, spot_ref, arr, tree, inv, left, right, spots, sems,
):
    devices = arr_ref.shape[0]
    vecs, rows = field_ref.shape
    parts = LANES // vecs
    half = arr.shape[0] // devices
    leaves = rows // leaf
    levels = right_hbm.shape[0]
    loads = [
        pltpu.make_async_copy(inv_hbm, inv, sems.at[0]),
        pltpu.make_async_copy(right_hbm, right, sems.at[1]),
        pltpu.make_async_copy(left_hbm.at[pl.ds(0, local_levels)], left, sems.at[2]),
    ]
    for load in loads:
        load.start()
    for d in range(devices):
        pos = arr_ref[d, half : half + 8, :].astype(F32)
        high = pos[0:parts, :]
        low = pos[parts : 2 * parts, :]
        spot = jnp.where(high > 0.5, (high - 1.0) * DIGIT + low, float(rows)).astype(I32)
        spot_ref[parts * d : parts * (d + 1), :] = spot
    copy = pltpu.make_async_copy(spot_ref, spots, sems.at[3])
    copy.start()

    def widen(d, _):
        arr[rows_at(d * half, half), :] = arr_ref[d, pl.ds(0, half), :].astype(F32)
        return 0

    lax.fori_loop(0, devices, widen, 0)

    def clear(i, _):
        tree[rows_at(i * 128, 128), :] = jnp.zeros((128, LANES), F32)
        return 0

    lax.fori_loop(0, rows // 128, clear, 0)
    copy.wait()

    def place(d, _):
        for u in range(half):
            row = arr[pl.ds(d * half + u, 1), :]
            for q in range(parts):
                at = pl.ds(spots[parts * d + q, u], 1)
                tree[at, pl.ds(q * vecs, vecs)] = row[:, q * vecs : (q + 1) * vecs]
        return 0

    lax.fori_loop(0, devices, place, 0, unroll=PLACE_UNROLL)
    for load in loads:
        load.wait()
    for l in range(leaves):
        block = tree[l * leaf : (l + 1) * leaf, :].astype(BF16)
        turned = dot(inv[l], block).T
        total = turned[:vecs]
        for q in range(1, parts):
            total = total + turned[q * vecs : (q + 1) * vecs]
        field_ref[:, l * leaf : (l + 1) * leaf] = total
    for k in range(local_levels):
        size = leaf << k
        scale = 1.0 / math.sqrt(size)
        coeff = []
        for n in range(rows // size):
            at = slice(n * size, (n + 1) * size)
            part = dot_nt(field_ref[:, at].astype(BF16), right[k, :, at])
            coeff.append((part * scale).astype(BF16))
        for n in range(rows // size):
            at = slice(n * size, (n + 1) * size)
            field_ref[:, at] = field_ref[:, at] - dot(coeff[n ^ 1], left[k, :, at])
    rounded = field_ref[...].astype(BF16)
    cross = levels - local_levels
    b = jnp.concatenate([dot_nt(rounded, right[k]) for k in range(local_levels, levels)], axis=1)
    gram = [gram_ref[j * rank : (j + 1) * rank, :] for j in range(cross)]
    pack_bands(message_ref, b, gram, rank, vecs // rank, cross)


def merge_kernel(bits, rank, scales, vecs, levels, *refs):
    group = 1 << bits
    p_ref = refs[group]
    halves = vecs // rank
    found = [unpack_bands(r[...].astype(F32), rank, halves, levels) for r in refs[:group]]
    b = [f[0] for f in found]
    gram = [f[1] for f in found]
    for step in range(bits):
        at = slice(step * rank, (step + 1) * rank)
        p = [(b[x ^ 1][:, at] * scales[step]).astype(BF16) for x in range(len(b))]
        p_ref[:, at] = p[0]
        if step + 1 < levels:
            b = [b[x] - dot(p[x], gram[x][step].astype(BF16)) for x in range(len(b))]
            b = [b[x] + b[x + 1] for x in range(0, len(b), 2)]
            gram = [
                [u + v for u, v in zip(gram[x], gram[x + 1])] for x in range(0, len(gram), 2)
            ]
    if levels > bits:
        keep = slice(bits * rank, levels * rank)
        rest = [g[:, keep] for g in gram[0][bits:]]
        pack_bands(refs[group + 1], b[0][:, keep], rest, rank, halves, levels - bits)


def back_kernel(first, rank, n_solved, field_ref, left, spot_ref, *refs):
    solved = refs[:n_solved]
    out_ref, done, spots, packed, sem = refs[n_solved:]
    devices, half, _ = out_ref.shape
    vecs, rows = field_ref.shape
    parts = LANES // vecs
    levels = left.shape[0]
    copy = pltpu.make_async_copy(spot_ref, spots, sem)
    copy.start()
    p = jnp.concatenate([r[...] for r in solved], axis=1)
    wide = 512
    for c in range(rows // wide):
        at = slice(c * wide, (c + 1) * wide)
        basis = jnp.concatenate([left[k, :, at] for k in range(first, levels)], axis=0)
        field = field_ref[:, at] - dot(p, basis)
        for q in range(wide // LANES):
            x = field[:, q * LANES : (q + 1) * LANES]
            low = c * wide + q * LANES
            done[low : low + LANES, :] = jnp.concatenate([x] * parts, axis=0).T
    copy.wait()
    group = iota((1, LANES), 1) // vecs

    def pick(d, _):
        for u in range(half):
            row = done[pl.ds(spots[parts * d, u], 1), :]
            for q in range(1, parts):
                row = jnp.where(group == q, done[pl.ds(spots[parts * d + q, u], 1), :], row)
            packed[pl.ds(d * half + u, 1), :] = row
        return 0

    lax.fori_loop(0, devices, pick, 0, unroll=PICK_UNROLL)

    def narrow(d, _):
        out_ref[d, :, :] = packed[rows_at(d * half, half), :].astype(BF16)
        return 0

    lax.fori_loop(0, devices, narrow, 0)


def final_kernel(ret_ref, row_ref, part_ref, out_ref, ret, picked, places, sem):
    devices, half, _ = ret_ref.shape
    vecs = out_ref.shape[0]
    parts = LANES // vecs
    blocks = row_ref.shape[0]
    copy = pltpu.make_async_copy(row_ref, places, sem)
    copy.start()

    def widen(d, _):
        ret[rows_at(d * half, half), :] = ret_ref[d, :, :].astype(F32)
        return 0

    lax.fori_loop(0, devices, widen, 0)
    copy.wait()

    def move(b, _):
        for u in range(LANES):
            picked[pl.ds(b * LANES + u, 1), :] = ret[pl.ds(places[b, u], 1), :]
        return 0

    lax.fori_loop(0, blocks, move, 0, unroll=FINAL_UNROLL)
    for b in range(blocks):
        x = picked[b * LANES : (b + 1) * LANES, :].T
        part = part_ref[b : b + 1, :]
        value = jnp.zeros((vecs, LANES), F32)
        for q in range(parts):
            value = jnp.where(part == q, x[q * vecs : (q + 1) * vecs], value)
        out_ref[:, b * LANES : (b + 1) * LANES] = value.astype(BF16)


def full(shape, dtype):
    return jax.ShapeDtypeStruct(shape, dtype)


def vmem():
    return pl.BlockSpec(memory_space=VMEM)


def hbm():
    return pl.BlockSpec(memory_space=pltpu.HBM)


def call(kernel, name, mib, flops, out_shape, in_specs, out_specs, scratch_shapes=()):
    return pl.pallas_call(
        kernel,
        out_shape=out_shape,
        in_specs=in_specs,
        out_specs=out_specs,
        scratch_shapes=scratch_shapes,
        compiler_params=pltpu.CompilerParams(vmem_limit_bytes=mib << 20),
        cost_estimate=pl.CostEstimate(flops=flops, bytes_accessed=1 << 20, transcendentals=0),
        name=name,
    )


def stay(x):
    return pltpu.with_memory_space_constraint(x, pltpu.HBM)


def flipped(block, axes, mask):
    count = lax.axis_size(axes)
    return lax.ppermute(block, axes, [(i, i ^ mask) for i in range(count)])


def body(vectors, row_counts, tree_slot, leaf_inverse, left_basis, right_basis):
    vecs, slots = vectors.shape
    leaves, leaf = leaf_inverse.shape[0], leaf_inverse.shape[1]
    rows = leaves * leaf
    levels, rank = left_basis.shape[0], left_basis.shape[1]
    n_leaf = lax.axis_size("leaf")
    n_sub = lax.axis_size("sub")
    devices = n_leaf * n_sub
    cross = devices.bit_length() - 1
    local_levels = levels - cross
    cap = (slots + devices - 1) // devices
    blocks = slots // LANES
    axes = ("leaf", "sub")
    parts = LANES // vecs
    half = ((cap + parts - 1) // parts + 7) // 8 * 8
    if vecs * 2 != LANES or half > LANES or slots % (2 * LANES) or rows & (rows - 1):
        raise ValueError("unsupported sizes")
    if rows // 256 > blocks // 2 or devices != 1 << cross:
        raise ValueError("unsupported sizes")

    outgoing, row_of, part_of, gram = call(
        functools.partial(send_kernel, rows, vecs, half, n_sub, local_levels),
        "send",
        20,
        1 << 30,
        (
            full((devices, half + 8, LANES), BF16),
            full((blocks, LANES), I32),
            full((blocks, LANES), I32),
            full((cross * rank, cross * rank), F32),
        ),
        [hbm()] * 5,
        (vmem(),) * 4,
        [
            SMEM((devices,), I32),
            VMEM((vecs, slots), BF16),
            VMEM((blocks, LANES), I32),
            VMEM((cross, rank, rows), BF16),
            VMEM((cross, rank, rows), BF16),
            VMEM((slots, LANES), F32),
            VMEM((devices * parts * half + 8, LANES), F32),
            VMEM((blocks, LANES), I32),
            SMEM((blocks, LANES), I32),
            VMEM((blocks, LANES), I32),
            VMEM((blocks, LANES), I32),
            VMEM((2 * devices, parts * LANES), F32),
            VMEM((8 * devices, LANES), F32),
            pltpu.SemaphoreType.DMA((6,)),
        ],
    )(*map(stay, (row_counts, vectors, tree_slot.reshape(blocks, LANES), left_basis, right_basis)))

    def exchange(x):
        return lax.all_to_all(x, axes, split_axis=0, concat_axis=0, tiled=True)

    arrived = exchange(outgoing)
    halves = vecs // rank
    field, message, spots = call(
        functools.partial(tree_kernel, local_levels, leaf, rank),
        "tree",
        20,
        1 << 30,
        (
            full((vecs, rows), F32),
            full((band_rows(halves, cross, rank), LANES), BF16),
            full((parts * devices, LANES), I32),
        ),
        [vmem(), hbm(), hbm(), hbm(), vmem()],
        (vmem(), vmem(), vmem()),
        [
            VMEM((devices * half, LANES), F32),
            VMEM((rows + 8, LANES), F32),
            VMEM((leaves, leaf, leaf), BF16),
            VMEM((local_levels, rank, rows), BF16),
            VMEM((levels, rank, rows), BF16),
            SMEM((parts * devices, LANES), I32),
            pltpu.SemaphoreType.DMA((4,)),
        ],
    )(arrived, stay(leaf_inverse), stay(left_basis), stay(right_basis), gram)

    solved = []
    bit = 0
    while bit < cross:
        take = 1 if (cross - bit) % 2 else 2
        level = local_levels + bit
        group = [message] + [flipped(message, axes, m << bit) for m in range(1, 1 << take)]
        scales = [1.0 / math.sqrt(leaf << (level + s)) for s in range(take)]
        left_over = cross - bit - take
        shapes = [full((vecs, take * rank), BF16)]
        if left_over:
            shapes.append(full((band_rows(halves, left_over, rank), LANES), BF16))
        out = call(
            functools.partial(merge_kernel, take, rank, scales, vecs, cross - bit),
            "merge",
            4,
            1 << 24,
            tuple(shapes),
            [vmem()] * len(group),
            (vmem(),) * len(shapes),
        )(*group)
        solved.append(out[0])
        message = out[-1]
        bit += take

    back = call(
        functools.partial(back_kernel, local_levels, rank, len(solved)),
        "back",
        14,
        1 << 30,
        full((devices, half, LANES), BF16),
        [vmem()] * (3 + len(solved)),
        vmem(),
        [
            VMEM((rows + 8, LANES), F32),
            SMEM((parts * devices, LANES), I32),
            VMEM((devices * half, LANES), F32),
            pltpu.SemaphoreType.DMA,
        ],
    )(field, left_basis, spots, *solved)
    returned = exchange(back)
    return call(
        final_kernel,
        "final",
        14,
        1 << 30,
        full((vecs, slots), BF16),
        [vmem(), vmem(), vmem()],
        vmem(),
        [
            VMEM((devices * half, LANES), F32),
            VMEM((slots, LANES), F32),
            SMEM((blocks, LANES), I32),
            pltpu.SemaphoreType.DMA,
        ],
    )(returned, row_of, part_of)


def solution(mesh):
    in_specs = (
        P(None, ("leaf", "sub")),
        P(),
        P(("leaf", "sub")),
        P(("leaf", "sub"), None, None),
        P(None, None, ("leaf", "sub")),
        P(None, None, ("leaf", "sub")),
    )
    out_specs = P(None, ("leaf", "sub"))
    return jax.shard_map(body, mesh=mesh, in_specs=in_specs, out_specs=out_specs, check_vma=False)
```

```python
import functools
import math

import jax
import jax.numpy as jnp
from jax import lax
from jax.experimental import pallas as pl
from jax.experimental.pallas import tpu as pltpu
from jax.sharding import PartitionSpec as P

F32 = jnp.float32
BF16 = jnp.bfloat16
I32 = jnp.int32
LANES = 128
DIGIT = 64
NT = (((1,), (1,)), ((), ()))
VMEM = pltpu.VMEM
SMEM = pltpu.SMEM
SEGMENTS = 8
PLACE_UNROLL = 32
PICK_UNROLL = 32
SEND_UNROLL = 40


def dot(a, b):
    return jnp.dot(a, b, preferred_element_type=F32)


def dot_nt(a, b):
    return lax.dot_general(a, b, NT, preferred_element_type=F32)


def iota(shape, dim):
    return lax.broadcasted_iota(I32, shape, dim)


def rows_at(start, size):
    return pl.ds(pl.multiple_of(start, 8), size)


def send_kernel(
    rows, vecs, half, n_sub, first, counts_hbm, vec_hbm, slot_hbm, left_hbm, right_hbm,
    out_ref, row_ref, part_ref, gram_ref,
    counts, vec, slots, left, right, xt, staged, flat, places, owners, codes, posf, sems,
):
    devices = out_ref.shape[0]
    parts = LANES // vecs
    blocks = slots.shape[0]
    levels = left_hbm.shape[0]
    cross = levels - first
    loads = [
        pltpu.make_async_copy(counts_hbm, counts, sems.at[0]),
        pltpu.make_async_copy(slot_hbm, slots, sems.at[1]),
        pltpu.make_async_copy(vec_hbm, vec, sems.at[2]),
        pltpu.make_async_copy(left_hbm.at[pl.ds(first, cross)], left, sems.at[3]),
        pltpu.make_async_copy(right_hbm.at[pl.ds(first, cross)], right, sems.at[4]),
    ]
    for load in loads:
        load.start()
    trash = devices * parts * half
    shift = rows.bit_length() - 1
    owner_id = iota((devices, LANES), 0)
    before = (iota((LANES, LANES), 0) < iota((LANES, LANES), 1)).astype(BF16)
    ones = jnp.ones((LANES, LANES), BF16)
    carry = jnp.zeros((devices, LANES), F32)
    for load in loads[:3]:
        load.wait()
    count = counts[lax.axis_index("leaf") * n_sub + lax.axis_index("sub")]
    for b in range(blocks):
        x = vec[:, b * LANES : (b + 1) * LANES].astype(F32)
        xt[b * LANES : (b + 1) * LANES, :] = jnp.concatenate([x] * parts, axis=0).T
        slot = slots[b : b + 1, :]
        lane = iota((1, LANES), 1) + b * LANES
        live = (lane < count) & (slot >= 0)
        owner = jnp.where(live, slot >> shift, -1)
        hot = owner_id == owner
        hot_b = jnp.where(hot, 1.0, 0.0).astype(BF16)
        ranks = dot(hot_b, before) + carry
        carry = carry + dot(hot_b, ones)
        rank = jnp.sum(jnp.where(hot, ranks, 0.0), axis=0, keepdims=True).astype(I32)
        flat[b : b + 1, :] = jnp.where(live, owner * (parts * half) + rank, trash)
        part = jnp.zeros((1, LANES), I32)
        for q in range(1, parts):
            part = part + jnp.where(rank >= q * half, 1, 0)
        inner = rank - part * half
        row_ref[b : b + 1, :] = jnp.where(live, owner * half + inner, 0)
        part_ref[b : b + 1, :] = jnp.where(live, part, parts)
        owners[b : b + 1, :] = owner
        codes[b : b + 1, :] = part * LANES + inner
    copy = pltpu.make_async_copy(flat, places, sems.at[5])
    copy.start()
    for load in loads[3:]:
        load.wait()
    code_id = iota((parts * LANES, LANES), 0)

    total = jnp.zeros((2 * devices, parts * LANES), F32)
    for i in range(blocks // 2):
        digits, spread = [], []
        for b in (2 * i, 2 * i + 1):
            hot = owner_id == owners[b : b + 1, :]
            local = slots[b : b + 1, :] & (rows - 1)
            high = ((local >> 6) + 1).astype(F32)
            low = (local & (DIGIT - 1)).astype(F32)
            digits.append(
                jnp.concatenate([jnp.where(hot, high, 0.0), jnp.where(hot, low, 0.0)], axis=0)
            )
            spread.append(jnp.where(code_id == codes[b : b + 1, :], 1.0, 0.0))
        total = total + dot_nt(
            jnp.concatenate(digits, axis=1).astype(BF16),
            jnp.concatenate(spread, axis=1).astype(BF16),
        )
    for d in range(devices):
        for q in range(parts):
            at = slice(q * LANES, (q + 1) * LANES)
            posf[8 * d + q : 8 * d + q + 1, :] = total[d : d + 1, at]
            posf[8 * d + parts + q : 8 * d + parts + q + 1, :] = total[devices + d : devices + d + 1, at]
    lhs = jnp.concatenate([left[k] for k in range(cross - 1)], axis=0)
    rhs = jnp.concatenate([right[k] for k in range(1, cross)], axis=0)
    gram_ref[...] = dot_nt(lhs, rhs)
    copy.wait()

    def move(b, _):
        for u in range(LANES):
            staged[pl.ds(places[b, u], 1), :] = xt[pl.ds(b * LANES + u, 1), :]
        return 0

    lax.fori_loop(0, blocks, move, 0, unroll=SEND_UNROLL)
    group = iota((half, LANES), 1) // vecs

    def pack(d, _):
        packed = staged[rows_at(d * parts * half, half), :]
        for q in range(1, parts):
            packed = jnp.where(group == q, staged[rows_at((d * parts + q) * half, half), :], packed)
        out_ref[d, pl.ds(0, half), :] = packed.astype(BF16)
        out_ref[d, pl.ds(half, 8), :] = posf[rows_at(d * 8, 8), :].astype(BF16)
        return 0

    lax.fori_loop(0, devices, pack, 0)


def band_tiles(halves, levels):
    tiles = [("b", h, k) for k in range(levels) for h in range(halves)]
    return tiles + [("g", j, k) for j in range(levels) for k in range(j + 1, levels)]


def band_rows(halves, levels, rank):
    return (len(band_tiles(halves, levels)) + 3) // 4 * rank


def pack_bands(ref, b, gram, rank, halves, levels):
    tiles = band_tiles(halves, levels)
    blank = jnp.zeros((rank, rank), F32)
    for r in range(0, len(tiles), 4):
        band = []
        for kind, x, k in tiles[r : r + 4]:
            at = slice(k * rank, (k + 1) * rank)
            band.append(b[x * rank : (x + 1) * rank, at] if kind == "b" else gram[x][:, at])
        band += [blank] * (4 - len(band))
        ref[r // 4 * rank : (r // 4 + 1) * rank, :] = jnp.concatenate(band, axis=1).astype(BF16)


def unpack_bands(value, rank, halves, levels):
    tiles = band_tiles(halves, levels)
    found = {}
    for t, key in enumerate(tiles):
        found[key] = value[t // 4 * rank : (t // 4 + 1) * rank, t % 4 * rank : (t % 4 + 1) * rank]
    b = jnp.concatenate(
        [
            jnp.concatenate([found["b", h, k] for k in range(levels)], axis=1)
            for h in range(halves)
        ],
        axis=0,
    )
    blank = jnp.zeros((rank, rank), F32)
    gram = [
        jnp.concatenate([found["g", j, k] if k > j else blank for k in range(levels)], axis=1)
        for j in range(levels)
    ]
    return b, gram


def tree_kernel(
    local_levels, leaf, rank, arr_ref, inv_hbm, left_hbm, right_hbm, gram_ref,
    field_ref, message_ref, spot_ref, arr, tree, inv, left, right, spots, sems,
):
    devices = arr_ref.shape[0]
    vecs, rows = field_ref.shape
    parts = LANES // vecs
    half = arr.shape[0] // devices
    leaves = rows // leaf
    levels = right_hbm.shape[0]
    loads = [
        pltpu.make_async_copy(inv_hbm, inv, sems.at[0]),
        pltpu.make_async_copy(right_hbm, right, sems.at[1]),
        pltpu.make_async_copy(left_hbm.at[pl.ds(0, local_levels)], left, sems.at[2]),
    ]
    for load in loads:
        load.start()
    for d in range(devices):
        pos = arr_ref[d, half : half + 8, :].astype(F32)
        high = pos[0:parts, :]
        low = pos[parts : 2 * parts, :]
        spot = jnp.where(high > 0.5, (high - 1.0) * DIGIT + low, float(rows)).astype(I32)
        spot_ref[parts * d : parts * (d + 1), :] = spot
    copy = pltpu.make_async_copy(spot_ref, spots, sems.at[3])
    copy.start()

    def widen(d, _):
        arr[rows_at(d * half, half), :] = arr_ref[d, pl.ds(0, half), :].astype(F32)
        return 0

    lax.fori_loop(0, devices, widen, 0)

    def clear(i, _):
        tree[rows_at(i * 128, 128), :] = jnp.zeros((128, LANES), F32)
        return 0

    lax.fori_loop(0, rows // 128, clear, 0)
    copy.wait()

    def place(d, _):
        for u in range(half):
            row = arr[pl.ds(d * half + u, 1), :]
            for q in range(parts):
                at = pl.ds(spots[parts * d + q, u], 1)
                tree[at, pl.ds(q * vecs, vecs)] = row[:, q * vecs : (q + 1) * vecs]
        return 0

    lax.fori_loop(0, devices, place, 0, unroll=PLACE_UNROLL)
    for load in loads:
        load.wait()
    for l in range(leaves):
        block = tree[l * leaf : (l + 1) * leaf, :].astype(BF16)
        turned = dot(inv[l], block).T
        total = turned[:vecs]
        for q in range(1, parts):
            total = total + turned[q * vecs : (q + 1) * vecs]
        field_ref[:, l * leaf : (l + 1) * leaf] = total
    for k in range(local_levels):
        size = leaf << k
        scale = 1.0 / math.sqrt(size)
        coeff = []
        for n in range(rows // size):
            at = slice(n * size, (n + 1) * size)
            part = dot_nt(field_ref[:, at].astype(BF16), right[k, :, at])
            coeff.append((part * scale).astype(BF16))
        for n in range(rows // size):
            at = slice(n * size, (n + 1) * size)
            field_ref[:, at] = field_ref[:, at] - dot(coeff[n ^ 1], left[k, :, at])
    rounded = field_ref[...].astype(BF16)
    cross = levels - local_levels
    b = dot_nt(rounded, jnp.concatenate([right[k] for k in range(local_levels, levels)], axis=0))
    blank = jnp.zeros((rank, rank), F32)
    gram = [
        jnp.concatenate([blank, gram_ref[j * rank : (j + 1) * rank, :]], axis=1)
        for j in range(cross - 1)
    ]
    pack_bands(message_ref, b, gram, rank, vecs // rank, cross)


def merge(messages, rank, scales, vecs, levels):
    halves = vecs // rank
    found = [unpack_bands(m.astype(F32), rank, halves, levels) for m in messages]
    b = [f[0] for f in found]
    gram = [f[1] for f in found]
    solved = []
    for step, scale in enumerate(scales):
        at = slice(step * rank, (step + 1) * rank)
        p = [(b[x ^ 1][:, at] * scale).astype(BF16) for x in range(len(b))]
        solved.append(p[0])
        if step + 1 < levels:
            b = [b[x] - dot(p[x], gram[x][step].astype(BF16)) for x in range(len(b))]
            b = [b[x] + b[x + 1] for x in range(0, len(b), 2)]
            gram = [
                [u + v for u, v in zip(gram[x], gram[x + 1])] for x in range(0, len(gram), 2)
            ]
    return solved, b[0], gram[0]


def merge_kernel(rank, scales, vecs, levels, *refs):
    bits = len(scales)
    messages, (p_ref, out_ref) = refs[:-2], refs[-2:]
    solved, b, gram = merge([r[...] for r in messages], rank, scales, vecs, levels)
    for step in range(bits):
        p_ref[:, step * rank : (step + 1) * rank] = solved[step]
    keep = slice(bits * rank, levels * rank)
    rest = [g[:, keep] for g in gram[bits:]]
    pack_bands(out_ref, b[:, keep], rest, rank, vecs // rank, levels - bits)


def back_kernel(first, rank, scales, n_solved, field_ref, left, spot_ref, *refs):
    out_ref, done, spots, packed, sem = refs[-5:]
    messages = [r[...] for r in refs[n_solved:-5]]
    devices, half, _ = out_ref.shape
    vecs, rows = field_ref.shape
    parts = LANES // vecs
    levels = left.shape[0]
    copy = pltpu.make_async_copy(spot_ref, spots, sem)
    copy.start()
    last = merge(messages, rank, scales, vecs, len(scales))[0]
    p = jnp.concatenate([r[...] for r in refs[:n_solved]] + last, axis=1)
    wide = 512
    for c in range(rows // wide):
        at = slice(c * wide, (c + 1) * wide)
        basis = jnp.concatenate([left[k, :, at] for k in range(first, levels)], axis=0)
        field = field_ref[:, at] - dot(p, basis)
        for q in range(wide // LANES):
            x = field[:, q * LANES : (q + 1) * LANES]
            low = c * wide + q * LANES
            done[low : low + LANES, :] = jnp.concatenate([x] * parts, axis=0).T
    copy.wait()
    group = iota((1, LANES), 1) // vecs

    def pick(d, _):
        for u in range(half):
            row = done[pl.ds(spots[parts * d, u], 1), :]
            for q in range(1, parts):
                row = jnp.where(group == q, done[pl.ds(spots[parts * d + q, u], 1), :], row)
            packed[pl.ds(d * half + u, 1), :] = row
        return 0

    lax.fori_loop(0, devices, pick, 0, unroll=PICK_UNROLL)

    def narrow(d, _):
        out_ref[d, :, :] = packed[rows_at(d * half, half), :].astype(BF16)
        return 0

    lax.fori_loop(0, devices, narrow, 0)


def final_kernel(segments, ret_ref, row_ref, part_ref, out_hbm, ret, picked, out, places, sems):
    devices, half, _ = ret_ref.shape
    vecs = out.shape[0]
    parts = LANES // vecs
    blocks = row_ref.shape[0]
    copy = pltpu.make_async_copy(row_ref, places, sems.at[segments])
    copy.start()

    def widen(d, _):
        ret[rows_at(d * half, half), :] = ret_ref[d, :, :].astype(F32)
        return 0

    lax.fori_loop(0, devices, widen, 0)
    copy.wait()

    def move(b, _):
        for u in range(LANES):
            picked[pl.ds(b * LANES + u, 1), :] = ret[pl.ds(places[b, u], 1), :]
        return 0

    def turn(b):
        x = picked[b * LANES : (b + 1) * LANES, :].T
        part = part_ref[b : b + 1, :]
        value = x[:vecs]
        for q in range(1, parts):
            value = jnp.where(part == q, x[q * vecs : (q + 1) * vecs], value)
        value = jnp.where(part == parts, 0.0, value)
        out[:, b * LANES : (b + 1) * LANES] = value.astype(BF16)

    per = blocks // segments
    stores = []
    for g in range(segments + 1):
        if g < segments:
            lax.fori_loop(g * per, (g + 1) * per, move, 0, unroll=per)
        if g > 0:
            for b in range((g - 1) * per, g * per):
                turn(b)
            at = pl.ds((g - 1) * per * LANES, per * LANES)
            stores.append(pltpu.make_async_copy(out.at[:, at], out_hbm.at[:, at], sems.at[g - 1]))
            stores[-1].start()
    for store in stores:
        store.wait()


def full(shape, dtype):
    return jax.ShapeDtypeStruct(shape, dtype)


def vmem():
    return pl.BlockSpec(memory_space=VMEM)


def hbm():
    return pl.BlockSpec(memory_space=pltpu.HBM)


def call(kernel, name, mib, flops, out_shape, in_specs, out_specs, scratch_shapes=()):
    return pl.pallas_call(
        kernel,
        out_shape=out_shape,
        in_specs=in_specs,
        out_specs=out_specs,
        scratch_shapes=scratch_shapes,
        compiler_params=pltpu.CompilerParams(vmem_limit_bytes=mib << 20),
        cost_estimate=pl.CostEstimate(flops=flops, bytes_accessed=1 << 20, transcendentals=0),
        name=name,
    )


def stay(x):
    return pltpu.with_memory_space_constraint(x, pltpu.HBM)


def flipped(block, axes, mask):
    count = lax.axis_size(axes)
    return lax.ppermute(block, axes, [(i, i ^ mask) for i in range(count)])


def body(vectors, row_counts, tree_slot, leaf_inverse, left_basis, right_basis):
    vecs, slots = vectors.shape
    leaves, leaf = leaf_inverse.shape[0], leaf_inverse.shape[1]
    rows = leaves * leaf
    levels, rank = left_basis.shape[0], left_basis.shape[1]
    n_leaf = lax.axis_size("leaf")
    n_sub = lax.axis_size("sub")
    devices = n_leaf * n_sub
    cross = devices.bit_length() - 1
    local_levels = levels - cross
    cap = (slots + devices - 1) // devices
    blocks = slots // LANES
    axes = ("leaf", "sub")
    parts = LANES // vecs
    half = ((cap + parts - 1) // parts + 7) // 8 * 8
    if vecs * 2 != LANES or half > LANES or slots % (2 * LANES) or rows & (rows - 1):
        raise ValueError("unsupported sizes")
    if rows // 256 > blocks // 2 or devices != 1 << cross:
        raise ValueError("unsupported sizes")

    outgoing, row_of, part_of, gram = call(
        functools.partial(send_kernel, rows, vecs, half, n_sub, local_levels),
        "send",
        20,
        1 << 30,
        (
            full((devices, half + 8, LANES), BF16),
            full((blocks, LANES), I32),
            full((blocks, LANES), I32),
            full(((cross - 1) * rank, (cross - 1) * rank), F32),
        ),
        [hbm()] * 5,
        (vmem(),) * 4,
        [
            SMEM((devices,), I32),
            VMEM((vecs, slots), BF16),
            VMEM((blocks, LANES), I32),
            VMEM((cross, rank, rows), BF16),
            VMEM((cross, rank, rows), BF16),
            VMEM((slots, LANES), F32),
            VMEM((devices * parts * half + 8, LANES), F32),
            VMEM((blocks, LANES), I32),
            SMEM((blocks, LANES), I32),
            VMEM((blocks, LANES), I32),
            VMEM((blocks, LANES), I32),
            VMEM((8 * devices, LANES), F32),
            pltpu.SemaphoreType.DMA((6,)),
        ],
    )(*map(stay, (row_counts, vectors, tree_slot.reshape(blocks, LANES), left_basis, right_basis)))

    def exchange(x):
        return lax.all_to_all(x, axes, split_axis=0, concat_axis=0, tiled=True)

    arrived = exchange(outgoing)
    halves = vecs // rank
    field, message, spots = call(
        functools.partial(tree_kernel, local_levels, leaf, rank),
        "tree",
        20,
        1 << 30,
        (
            full((vecs, rows), F32),
            full((band_rows(halves, cross, rank), LANES), BF16),
            full((parts * devices, LANES), I32),
        ),
        [vmem(), hbm(), hbm(), hbm(), vmem()],
        (vmem(), vmem(), vmem()),
        [
            VMEM((devices * half, LANES), F32),
            VMEM((rows + 8, LANES), F32),
            VMEM((leaves, leaf, leaf), BF16),
            VMEM((local_levels, rank, rows), BF16),
            VMEM((levels, rank, rows), BF16),
            SMEM((parts * devices, LANES), I32),
            pltpu.SemaphoreType.DMA((4,)),
        ],
    )(arrived, stay(leaf_inverse), stay(left_basis), stay(right_basis), gram)

    solved = []
    bit = 0
    while bit < cross:
        take = 1 if (cross - bit) % 2 else 2
        level = local_levels + bit
        group = [message] + [flipped(message, axes, m << bit) for m in range(1, 1 << take)]
        scales = [1.0 / math.sqrt(leaf << (level + s)) for s in range(take)]
        left_over = cross - bit - take
        bit += take
        if not left_over:
            break
        p, message = call(
            functools.partial(merge_kernel, rank, scales, vecs, left_over + take),
            "merge",
            4,
            1 << 24,
            (
                full((vecs, take * rank), BF16),
                full((band_rows(halves, left_over, rank), LANES), BF16),
            ),
            [vmem()] * len(group),
            (vmem(),) * 2,
        )(*group)
        solved.append(p)

    back = call(
        functools.partial(back_kernel, local_levels, rank, scales, len(solved)),
        "back",
        14,
        1 << 30,
        full((devices, half, LANES), BF16),
        [vmem()] * (3 + len(solved) + len(group)),
        vmem(),
        [
            VMEM((rows + 8, LANES), F32),
            SMEM((parts * devices, LANES), I32),
            VMEM((devices * half, LANES), F32),
            pltpu.SemaphoreType.DMA,
        ],
    )(field, left_basis, spots, *solved, *group)
    returned = exchange(back)
    segments = SEGMENTS if blocks % SEGMENTS == 0 else 1
    return call(
        functools.partial(final_kernel, segments),
        "final",
        14,
        1 << 30,
        full((vecs, slots), BF16),
        [vmem(), vmem(), vmem()],
        hbm(),
        [
            VMEM((devices * half, LANES), F32),
            VMEM((slots, LANES), F32),
            VMEM((vecs, slots), BF16),
            SMEM((blocks, LANES), I32),
            pltpu.SemaphoreType.DMA((segments + 1,)),
        ],
    )(returned, row_of, part_of)


def solution(mesh):
    in_specs = (
        P(None, ("leaf", "sub")),
        P(),
        P(("leaf", "sub")),
        P(("leaf", "sub"), None, None),
        P(None, None, ("leaf", "sub")),
        P(None, None, ("leaf", "sub")),
    )
    out_specs = P(None, ("leaf", "sub"))
    return jax.shard_map(body, mesh=mesh, in_specs=in_specs, out_specs=out_specs, check_vma=False)
```

```python
import functools
import math

import jax
import jax.numpy as jnp
from jax import lax
from jax.experimental import pallas as pl
from jax.experimental.pallas import tpu as pltpu
from jax.sharding import PartitionSpec as P

F32 = jnp.float32
BF16 = jnp.bfloat16
I32 = jnp.int32
LANES = 128
DIGIT = 64
NT = (((1,), (1,)), ((), ()))
VMEM = pltpu.VMEM
SMEM = pltpu.SMEM
SEGMENTS = 8
PLACE_UNROLL = 32
PICK_UNROLL = 32
SEND_UNROLL = 40


def dot(a, b):
    return jnp.dot(a, b, preferred_element_type=F32)


def dot_nt(a, b):
    return lax.dot_general(a, b, NT, preferred_element_type=F32)


def iota(shape, dim):
    return lax.broadcasted_iota(I32, shape, dim)


def rows_at(start, size):
    return pl.ds(pl.multiple_of(start, 8), size)


def send_kernel(
    rows, vecs, half, n_sub, first, counts_hbm, vec_hbm, slot_hbm, left_hbm, right_hbm,
    out_ref, row_ref, part_ref, gram_ref,
    counts, vec, slots, left, right, xt, staged, flat, places, owners, codes, posf, sems,
):
    devices = out_ref.shape[0]
    parts = LANES // vecs
    blocks = slots.shape[0]
    levels = left_hbm.shape[0]
    cross = levels - first
    loads = [
        pltpu.make_async_copy(counts_hbm, counts, sems.at[0]),
        pltpu.make_async_copy(slot_hbm, slots, sems.at[1]),
        pltpu.make_async_copy(vec_hbm, vec, sems.at[2]),
        pltpu.make_async_copy(left_hbm.at[pl.ds(first, cross)], left, sems.at[3]),
        pltpu.make_async_copy(right_hbm.at[pl.ds(first, cross)], right, sems.at[4]),
    ]
    for load in loads:
        load.start()
    trash = devices * parts * half
    shift = rows.bit_length() - 1
    owner_id = iota((devices, LANES), 0)
    before = (iota((LANES, LANES), 0) < iota((LANES, LANES), 1)).astype(BF16)
    ones = jnp.ones((LANES, LANES), BF16)
    carry = jnp.zeros((devices, LANES), F32)
    for load in loads[:3]:
        load.wait()
    count = counts[lax.axis_index("leaf") * n_sub + lax.axis_index("sub")]
    for b in range(blocks):
        x = vec[:, b * LANES : (b + 1) * LANES].astype(F32)
        xt[b * LANES : (b + 1) * LANES, :] = jnp.concatenate([x] * parts, axis=0).T
        slot = slots[b : b + 1, :]
        lane = iota((1, LANES), 1) + b * LANES
        live = (lane < count) & (slot >= 0)
        owner = jnp.where(live, slot >> shift, -1)
        hot = owner_id == owner
        hot_b = jnp.where(hot, 1.0, 0.0).astype(BF16)
        ranks = dot(hot_b, before) + carry
        carry = carry + dot(hot_b, ones)
        rank = jnp.sum(jnp.where(hot, ranks, 0.0), axis=0, keepdims=True).astype(I32)
        flat[b : b + 1, :] = jnp.where(live, owner * (parts * half) + rank, trash)
        part = jnp.zeros((1, LANES), I32)
        for q in range(1, parts):
            part = part + jnp.where(rank >= q * half, 1, 0)
        inner = rank - part * half
        row_ref[b : b + 1, :] = jnp.where(live, owner * half + inner, 0)
        part_ref[b : b + 1, :] = jnp.where(live, part, parts)
        owners[b : b + 1, :] = owner
        codes[b : b + 1, :] = part * LANES + inner
    copy = pltpu.make_async_copy(flat, places, sems.at[5])
    copy.start()
    for load in loads[3:]:
        load.wait()
    code_id = iota((parts * LANES, LANES), 0)

    total = jnp.zeros((2 * devices, parts * LANES), F32)
    for i in range(blocks // 2):
        digits, spread = [], []
        for b in (2 * i, 2 * i + 1):
            hot = owner_id == owners[b : b + 1, :]
            local = slots[b : b + 1, :] & (rows - 1)
            high = ((local >> 6) + 1).astype(F32)
            low = (local & (DIGIT - 1)).astype(F32)
            digits.append(
                jnp.concatenate([jnp.where(hot, high, 0.0), jnp.where(hot, low, 0.0)], axis=0)
            )
            spread.append(jnp.where(code_id == codes[b : b + 1, :], 1.0, 0.0))
        total = total + dot_nt(
            jnp.concatenate(digits, axis=1).astype(BF16),
            jnp.concatenate(spread, axis=1).astype(BF16),
        )
    for d in range(devices):
        for q in range(parts):
            at = slice(q * LANES, (q + 1) * LANES)
            posf[8 * d + q : 8 * d + q + 1, :] = total[d : d + 1, at]
            posf[8 * d + parts + q : 8 * d + parts + q + 1, :] = total[devices + d : devices + d + 1, at]
    lhs = jnp.concatenate([left[k] for k in range(cross - 1)], axis=0)
    rhs = jnp.concatenate([right[k] for k in range(1, cross)], axis=0)
    gram_ref[...] = dot_nt(lhs, rhs)
    copy.wait()

    def move(b, _):
        for u in range(LANES):
            staged[pl.ds(places[b, u], 1), :] = xt[pl.ds(b * LANES + u, 1), :]
        return 0

    lax.fori_loop(0, blocks, move, 0, unroll=SEND_UNROLL)
    group = iota((half, LANES), 1) // vecs

    def pack(d, _):
        packed = staged[rows_at(d * parts * half, half), :]
        for q in range(1, parts):
            packed = jnp.where(group == q, staged[rows_at((d * parts + q) * half, half), :], packed)
        out_ref[d, pl.ds(0, half), :] = packed.astype(BF16)
        out_ref[d, pl.ds(half, 8), :] = posf[rows_at(d * 8, 8), :].astype(BF16)
        return 0

    lax.fori_loop(0, devices, pack, 0)


def band_tiles(halves, levels):
    tiles = [("b", h, k) for k in range(levels) for h in range(halves)]
    return tiles + [("g", j, k) for j in range(levels) for k in range(j + 1, levels)]


def band_rows(halves, levels, rank):
    return (len(band_tiles(halves, levels)) + 3) // 4 * rank


def pack_bands(ref, b, gram, rank, halves, levels):
    tiles = band_tiles(halves, levels)
    blank = jnp.zeros((rank, rank), F32)
    for r in range(0, len(tiles), 4):
        band = []
        for kind, x, k in tiles[r : r + 4]:
            at = slice(k * rank, (k + 1) * rank)
            band.append(b[x * rank : (x + 1) * rank, at] if kind == "b" else gram[x][:, at])
        band += [blank] * (4 - len(band))
        ref[r // 4 * rank : (r // 4 + 1) * rank, :] = jnp.concatenate(band, axis=1).astype(BF16)


def unpack_bands(value, rank, halves, levels):
    tiles = band_tiles(halves, levels)
    found = {}
    for t, key in enumerate(tiles):
        found[key] = value[t // 4 * rank : (t // 4 + 1) * rank, t % 4 * rank : (t % 4 + 1) * rank]
    b = jnp.concatenate(
        [
            jnp.concatenate([found["b", h, k] for k in range(levels)], axis=1)
            for h in range(halves)
        ],
        axis=0,
    )
    blank = jnp.zeros((rank, rank), F32)
    gram = [
        jnp.concatenate([found["g", j, k] if k > j else blank for k in range(levels)], axis=1)
        for j in range(levels)
    ]
    return b, gram


def tree_kernel(
    local_levels, leaf, rank, arr_ref, inv_hbm, left_hbm, right_hbm, gram_ref,
    field_ref, message_ref, spot_ref, arr, tree, tree_rows, inv, left, right, spots, sems,
):
    devices = arr_ref.shape[0]
    vecs, rows = field_ref.shape
    parts = LANES // vecs
    half = arr.shape[0] // devices
    leaves = rows // leaf
    levels = right_hbm.shape[0]
    loads = [
        pltpu.make_async_copy(inv_hbm, inv, sems.at[0]),
        pltpu.make_async_copy(right_hbm, right, sems.at[1]),
        pltpu.make_async_copy(left_hbm.at[pl.ds(0, local_levels)], left, sems.at[2]),
    ]
    for load in loads:
        load.start()
    for d in range(devices):
        pos = arr_ref[d, half : half + 8, :].astype(F32)
        high = pos[0:parts, :]
        low = pos[parts : 2 * parts, :]
        spot = jnp.where(high > 0.5, (high - 1.0) * DIGIT + low, float(rows)).astype(I32)
        spot_ref[parts * d : parts * (d + 1), :] = spot
    copy = pltpu.make_async_copy(spot_ref, spots, sems.at[3])
    copy.start()

    def widen(d, _):
        arr[rows_at(d * half, half), :] = arr_ref[d, pl.ds(0, half), :].astype(F32)
        return 0

    lax.fori_loop(0, devices, widen, 0)

    def clear(i, _):
        tree[rows_at(i * 128, 128), :] = jnp.zeros((128, LANES), F32)
        return 0

    lax.fori_loop(0, rows // 128, clear, 0)
    copy.wait()

    def place(d, _):
        for u in range(half):
            row = arr[pl.ds(d * half + u, 1), :]
            for q in range(parts):
                at = pl.ds(spots[parts * d + q, u], 1)
                tree[at, pl.ds(q * vecs, vecs)] = row[:, q * vecs : (q + 1) * vecs]
        return 0

    lax.fori_loop(0, devices, place, 0, unroll=PLACE_UNROLL)
    for load in loads:
        load.wait()
    products = tree_rows
    for l in range(leaves):
        at = slice(l * leaf, (l + 1) * leaf)
        products[at, :] = dot(inv[l], tree[at, :].astype(BF16))
    for l in range(leaves):
        turned = products[l * leaf : (l + 1) * leaf, :].T
        total = turned[:vecs]
        for q in range(1, parts):
            total = total + turned[q * vecs : (q + 1) * vecs]
        field_ref[:, l * leaf : (l + 1) * leaf] = total
    for k in range(local_levels):
        size = leaf << k
        scale = 1.0 / math.sqrt(size)
        coeff = []
        for n in range(rows // size):
            at = slice(n * size, (n + 1) * size)
            part = dot_nt(field_ref[:, at].astype(BF16), right[k, :, at])
            coeff.append((part * scale).astype(BF16))
        for n in range(rows // size):
            at = slice(n * size, (n + 1) * size)
            field_ref[:, at] = field_ref[:, at] - dot(coeff[n ^ 1], left[k, :, at])
    rounded = field_ref[...].astype(BF16)
    cross = levels - local_levels
    b = dot_nt(rounded, jnp.concatenate([right[k] for k in range(local_levels, levels)], axis=0))
    blank = jnp.zeros((rank, rank), F32)
    gram = [
        jnp.concatenate([blank, gram_ref[j * rank : (j + 1) * rank, :]], axis=1)
        for j in range(cross - 1)
    ]
    pack_bands(message_ref, b, gram, rank, vecs // rank, cross)


def merge(messages, rank, scales, vecs, levels):
    halves = vecs // rank
    found = [unpack_bands(m.astype(F32), rank, halves, levels) for m in messages]
    b = [f[0] for f in found]
    gram = [f[1] for f in found]
    solved = []
    for step, scale in enumerate(scales):
        at = slice(step * rank, (step + 1) * rank)
        p = [(b[x ^ 1][:, at] * scale).astype(BF16) for x in range(len(b))]
        solved.append(p[0])
        if step + 1 < levels:
            b = [b[x] - dot(p[x], gram[x][step].astype(BF16)) for x in range(len(b))]
            b = [b[x] + b[x + 1] for x in range(0, len(b), 2)]
            gram = [
                [u + v for u, v in zip(gram[x], gram[x + 1])] for x in range(0, len(gram), 2)
            ]
    return solved, b[0], gram[0]


def merge_kernel(rank, scales, vecs, levels, *refs):
    bits = len(scales)
    messages, (p_ref, out_ref) = refs[:-2], refs[-2:]
    solved, b, gram = merge([r[...] for r in messages], rank, scales, vecs, levels)
    for step in range(bits):
        p_ref[:, step * rank : (step + 1) * rank] = solved[step]
    keep = slice(bits * rank, levels * rank)
    rest = [g[:, keep] for g in gram[bits:]]
    pack_bands(out_ref, b[:, keep], rest, rank, vecs // rank, levels - bits)


def back_kernel(first, rank, scales, n_solved, field_ref, left, spot_ref, *refs):
    out_ref, done, spots, packed, sem = refs[-5:]
    messages = [r[...] for r in refs[n_solved:-5]]
    devices, half, _ = out_ref.shape
    vecs, rows = field_ref.shape
    parts = LANES // vecs
    levels = left.shape[0]
    copy = pltpu.make_async_copy(spot_ref, spots, sem)
    copy.start()
    last = merge(messages, rank, scales, vecs, len(scales))[0]
    p = jnp.concatenate([r[...] for r in refs[:n_solved]] + last, axis=1)
    wide = 512
    for c in range(rows // wide):
        at = slice(c * wide, (c + 1) * wide)
        basis = jnp.concatenate([left[k, :, at] for k in range(first, levels)], axis=0)
        field = field_ref[:, at] - dot(p, basis)
        for q in range(wide // LANES):
            x = field[:, q * LANES : (q + 1) * LANES]
            low = c * wide + q * LANES
            done[low : low + LANES, :] = jnp.concatenate([x] * parts, axis=0).T
    copy.wait()
    group = iota((1, LANES), 1) // vecs

    def pick(d, _):
        for u in range(half):
            row = done[pl.ds(spots[parts * d, u], 1), :]
            for q in range(1, parts):
                row = jnp.where(group == q, done[pl.ds(spots[parts * d + q, u], 1), :], row)
            packed[pl.ds(d * half + u, 1), :] = row
        return 0

    lax.fori_loop(0, devices, pick, 0, unroll=PICK_UNROLL)

    def narrow(d, _):
        out_ref[d, :, :] = packed[rows_at(d * half, half), :].astype(BF16)
        return 0

    lax.fori_loop(0, devices, narrow, 0)


def final_kernel(segments, ret_ref, row_ref, part_ref, out_hbm, ret, picked, out, places, sems):
    devices, half, _ = ret_ref.shape
    vecs = out.shape[0]
    parts = LANES // vecs
    blocks = row_ref.shape[0]
    copy = pltpu.make_async_copy(row_ref, places, sems.at[segments])
    copy.start()

    def widen(d, _):
        ret[rows_at(d * half, half), :] = ret_ref[d, :, :].astype(F32)
        return 0

    lax.fori_loop(0, devices, widen, 0)
    copy.wait()

    def move(b, _):
        for u in range(LANES):
            picked[pl.ds(b * LANES + u, 1), :] = ret[pl.ds(places[b, u], 1), :]
        return 0

    def turn(b):
        x = picked[b * LANES : (b + 1) * LANES, :].T
        part = part_ref[b : b + 1, :]
        value = x[:vecs]
        for q in range(1, parts):
            value = jnp.where(part == q, x[q * vecs : (q + 1) * vecs], value)
        value = jnp.where(part == parts, 0.0, value)
        out[:, b * LANES : (b + 1) * LANES] = value.astype(BF16)

    per = blocks // segments
    stores = []
    for g in range(segments + 1):
        if g < segments:
            lax.fori_loop(g * per, (g + 1) * per, move, 0, unroll=per)
        if g > 0:
            for b in range((g - 1) * per, g * per):
                turn(b)
            at = pl.ds((g - 1) * per * LANES, per * LANES)
            stores.append(pltpu.make_async_copy(out.at[:, at], out_hbm.at[:, at], sems.at[g - 1]))
            stores[-1].start()
    for store in stores:
        store.wait()


def full(shape, dtype):
    return jax.ShapeDtypeStruct(shape, dtype)


def vmem():
    return pl.BlockSpec(memory_space=VMEM)


def hbm():
    return pl.BlockSpec(memory_space=pltpu.HBM)


def call(kernel, name, mib, flops, out_shape, in_specs, out_specs, scratch_shapes=()):
    return pl.pallas_call(
        kernel,
        out_shape=out_shape,
        in_specs=in_specs,
        out_specs=out_specs,
        scratch_shapes=scratch_shapes,
        compiler_params=pltpu.CompilerParams(vmem_limit_bytes=mib << 20),
        cost_estimate=pl.CostEstimate(flops=flops, bytes_accessed=1 << 20, transcendentals=0),
        name=name,
    )


def stay(x):
    return pltpu.with_memory_space_constraint(x, pltpu.HBM)


def flipped(block, axes, mask):
    count = lax.axis_size(axes)
    return lax.ppermute(block, axes, [(i, i ^ mask) for i in range(count)])


def body(vectors, row_counts, tree_slot, leaf_inverse, left_basis, right_basis):
    vecs, slots = vectors.shape
    leaves, leaf = leaf_inverse.shape[0], leaf_inverse.shape[1]
    rows = leaves * leaf
    levels, rank = left_basis.shape[0], left_basis.shape[1]
    n_leaf = lax.axis_size("leaf")
    n_sub = lax.axis_size("sub")
    devices = n_leaf * n_sub
    cross = devices.bit_length() - 1
    local_levels = levels - cross
    cap = (slots + devices - 1) // devices
    blocks = slots // LANES
    axes = ("leaf", "sub")
    parts = LANES // vecs
    half = ((cap + parts - 1) // parts + 7) // 8 * 8
    if vecs * 2 != LANES or half > LANES or slots % (2 * LANES) or rows & (rows - 1):
        raise ValueError("unsupported sizes")
    if rows // 256 > blocks // 2 or devices != 1 << cross:
        raise ValueError("unsupported sizes")

    outgoing, row_of, part_of, gram = call(
        functools.partial(send_kernel, rows, vecs, half, n_sub, local_levels),
        "send",
        20,
        1 << 30,
        (
            full((devices, half + 8, LANES), BF16),
            full((blocks, LANES), I32),
            full((blocks, LANES), I32),
            full(((cross - 1) * rank, (cross - 1) * rank), F32),
        ),
        [hbm()] * 5,
        (vmem(),) * 4,
        [
            SMEM((devices,), I32),
            VMEM((vecs, slots), BF16),
            VMEM((blocks, LANES), I32),
            VMEM((cross, rank, rows), BF16),
            VMEM((cross, rank, rows), BF16),
            VMEM((slots, LANES), F32),
            VMEM((devices * parts * half + 8, LANES), F32),
            VMEM((blocks, LANES), I32),
            SMEM((blocks, LANES), I32),
            VMEM((blocks, LANES), I32),
            VMEM((blocks, LANES), I32),
            VMEM((8 * devices, LANES), F32),
            pltpu.SemaphoreType.DMA((6,)),
        ],
    )(*map(stay, (row_counts, vectors, tree_slot.reshape(blocks, LANES), left_basis, right_basis)))

    def exchange(x):
        return lax.all_to_all(x, axes, split_axis=0, concat_axis=0, tiled=True)

    arrived = exchange(outgoing)
    halves = vecs // rank
    field, message, spots = call(
        functools.partial(tree_kernel, local_levels, leaf, rank),
        "tree",
        20,
        1 << 30,
        (
            full((vecs, rows), F32),
            full((band_rows(halves, cross, rank), LANES), BF16),
            full((parts * devices, LANES), I32),
        ),
        [vmem(), hbm(), hbm(), hbm(), vmem()],
        (vmem(), vmem(), vmem()),
        [
            VMEM((devices * half, LANES), F32),
            VMEM((rows + 8, LANES), F32),
            VMEM((rows, LANES), F32),
            VMEM((leaves, leaf, leaf), BF16),
            VMEM((local_levels, rank, rows), BF16),
            VMEM((levels, rank, rows), BF16),
            SMEM((parts * devices, LANES), I32),
            pltpu.SemaphoreType.DMA((4,)),
        ],
    )(arrived, stay(leaf_inverse), stay(left_basis), stay(right_basis), gram)

    solved = []
    bit = 0
    while bit < cross:
        take = 1 if (cross - bit) % 2 else 2
        level = local_levels + bit
        group = [message] + [flipped(message, axes, m << bit) for m in range(1, 1 << take)]
        scales = [1.0 / math.sqrt(leaf << (level + s)) for s in range(take)]
        left_over = cross - bit - take
        bit += take
        if not left_over:
            break
        p, message = call(
            functools.partial(merge_kernel, rank, scales, vecs, left_over + take),
            "merge",
            4,
            1 << 24,
            (
                full((vecs, take * rank), BF16),
                full((band_rows(halves, left_over, rank), LANES), BF16),
            ),
            [vmem()] * len(group),
            (vmem(),) * 2,
        )(*group)
        solved.append(p)

    back = call(
        functools.partial(back_kernel, local_levels, rank, scales, len(solved)),
        "back",
        14,
        1 << 30,
        full((devices, half, LANES), BF16),
        [vmem()] * (3 + len(solved) + len(group)),
        vmem(),
        [
            VMEM((rows + 8, LANES), F32),
            SMEM((parts * devices, LANES), I32),
            VMEM((devices * half, LANES), F32),
            pltpu.SemaphoreType.DMA,
        ],
    )(field, left_basis, spots, *solved, *group)
    returned = exchange(back)
    segments = SEGMENTS if blocks % SEGMENTS == 0 else 1
    return call(
        functools.partial(final_kernel, segments),
        "final",
        14,
        1 << 30,
        full((vecs, slots), BF16),
        [vmem(), vmem(), vmem()],
        hbm(),
        [
            VMEM((devices * half, LANES), F32),
            VMEM((slots, LANES), F32),
            VMEM((vecs, slots), BF16),
            SMEM((blocks, LANES), I32),
            pltpu.SemaphoreType.DMA((segments + 1,)),
        ],
    )(returned, row_of, part_of)


def solution(mesh):
    in_specs = (
        P(None, ("leaf", "sub")),
        P(),
        P(("leaf", "sub")),
        P(("leaf", "sub"), None, None),
        P(None, None, ("leaf", "sub")),
        P(None, None, ("leaf", "sub")),
    )
    out_specs = P(None, ("leaf", "sub"))
    return jax.shard_map(body, mesh=mesh, in_specs=in_specs, out_specs=out_specs, check_vma=False)
```
